256 devices in a mesh: gx: 4 (over z_lo), gy: 8 (over x, z_hi), gz: 8 (over y, core).
Axes of the slice: x: 4, y: 4, z: 8 (z_hi: 2, z_lo: 4; z = z_hi * 4 + z_lo), core: 2. Of those that a mesh axis runs over, the one named last changes fastest.
Arguments:
- attn_out: bfloat16 [16384, 8192], P('gx', ('gy', 'gz')), may hold values from -16 to 16
- out_grad: bfloat16 [16384, 8192], P('gx', ('gz', 'gy')), may hold values from -0.046875 to 0.046875
- valid_counts: int32 [16], P('gx'), may hold values from 128 to 1024
Outputs:
- weight_grad: float32 [8192, 8192], P(('gy', 'gx'), 'gz')
The draws below stay inside these ranges and needn't reach their ends.
Inputs may be any that keep to these rules, and one draw needn't show every extreme that they name: `valid_counts`: valid tokens of a packed row come first, padding after.
All inputs are finite; a program needn't handle non-finite values.
Results may differ from the reference program's by a relative error of at most 0.0003.
Values may be sent and summed in bfloat16 or wider, within the bound.
A program may use at most 64 MiB of HBM per device.

```python
import jax
import jax.numpy as jnp
from jax import lax

D = 8192
HD = 8192
SEQ = 1024
ROWS = 16
TOKENS = 16384


def set_ends(drawn, rng, smallest, high):
    place = [jax.random.randint(jax.random.fold_in(rng, axis), (), 0, length) for axis, length in enumerate(drawn.shape)]
    main_axis = drawn.shape.index(max(drawn.shape))
    beside = place[:main_axis] + [(place[main_axis] + 1) % drawn.shape[main_axis]] + place[main_axis + 1:]
    return drawn.at[tuple(place)].set(smallest).at[tuple(beside)].set(high)


def raised(values, key, source, target, shards_of, factor):
    owner, partner = [(jnp.arange(values.shape[position]) // (values.shape[position] // shards_of)).reshape([-1 if axis == position else 1 for axis in range(values.ndim)]) for position in (source, target)]
    chosen = jax.random.permutation(key, shards_of)[partner]
    strong = (owner == chosen) | (owner == (partner + shards_of // 2) % shards_of)
    return jnp.where(strong, factor * values, values)


def level_of(stream_key, shape, split, least, largest):
    factor_of = 1.0
    for position, blocks in split:
        draws = jax.random.uniform(jax.random.fold_in(jax.random.fold_in(stream_key, 6), position), (blocks,), jnp.float32, least / len(split), largest / len(split))
        factor_of = factor_of * jnp.repeat(jnp.exp(draws), shape[position] // blocks).reshape((-1,) + (1,) * (len(shape) - 1 - position))
    return factor_of


def scatter_about(stream_key, dims, spread, bound, shards=(), kind=jnp.bfloat16):
    factor_of = level_of(stream_key, dims, shards, -0.22, 0.18) if shards else 1.0
    result = jax.random.normal(stream_key, dims, jnp.float32) * spread * factor_of
    return jnp.minimum(jnp.maximum(result, -bound), bound).astype(kind)


def heavy_noise(rng, dims, deviation, reach, shards, heavy, kind=jnp.bfloat16):
    result = deviation * jax.random.normal(rng, dims, jnp.float32)
    if shards:
        result = result * level_of(rng, dims, shards, -0.22, 0.18)
    return jnp.clip(raised(result, jax.random.fold_in(rng, 3), *heavy), -reach, reach).astype(kind)


def setup_inputs(seed: int = 0) -> dict:
    arg_keys = jax.random.split(jax.random.key(seed), 4)
    attn_out = heavy_noise(arg_keys[0], (TOKENS, HD), 1.0, 16.0, ((0, 4), (1, 64)), (0, 1, 64, 4.0))
    out_grad = scatter_about(arg_keys[1], (TOKENS, D), (TOKENS ** -0.5), 0.046875, ((0, 4), (1, 64)))
    valid_counts = set_ends(jax.random.randint(arg_keys[2], (ROWS,), SEQ // 8, SEQ + 1), jax.random.fold_in(arg_keys[2], 1), SEQ // 8, SEQ).astype(jnp.int32)
    return {"attn_out": attn_out, "out_grad": out_grad, "valid_counts": valid_counts}


def reference(attn_out, out_grad, valid_counts):
    positions = jnp.arange(SEQ, dtype=jnp.int32)
    kept_rows = (positions[None, :] < valid_counts[:, None]).reshape(-1)
    masked = jnp.where(kept_rows[:, None], out_grad, jnp.zeros((), out_grad.dtype))
    return lax.dot_general(attn_out, masked, (((0,), (0,)), ((), ())), preferred_element_type=jnp.float32)
```

```python
import functools

import jax
import jax.numpy as jnp
from jax import lax
from jax.experimental import pallas as pl
from jax.experimental.pallas import tpu as pltpu
from jax.sharding import PartitionSpec as P

MESH = pl.DeviceIdType.MESH
TOK = 4096
SEQ = 1024
BLK = 128
CHK = TOK // 4
HALF = TOK // 2
COPIES = 64


def kernel(vc, a_hbm, b_hbm, out, raw, at, bb, sbuf, rbuf, ssc, rsc, lsem, ss, rs):
    zl = lax.axis_index("gx")
    gy = lax.axis_index("gy")
    gz = lax.axis_index("gz")
    x, zh = gy // 2, gy % 2
    y, c = gz // 2, gz % 2
    xr, xl, xo = (x + 1) % 4, (x + 3) % 4, (x + 2) % 4
    yr, yl, yo = (y + 1) % 4, (y + 3) % 4, (y + 2) % 4

    right, left = (zl, xr * 2 + zh, gz), (zl, xl * 2 + zh, gz)
    far = (zl, x * 2 + (1 - zh), gz)
    up, down = (zl, gy, yr * 2 + c), (zl, gy, yl * 2 + c)
    opposite = (zl, gy, yo * 2 + c)
    sibling = (zl, gy, y * 2 + (1 - c))
    owners = [((zl + d) % 4, gy, gz) for d in range(1, 4)]

    barrier = pltpu.get_barrier_semaphore()
    partners = [right, left, far, up, down, sibling] + owners
    for dev in partners:
        pl.semaphore_signal(barrier, inc=1, device_id=dev, device_id_type=MESH)

    load_a = pltpu.make_async_copy(a_hbm, raw, lsem.at[0])
    load_b = pltpu.make_async_copy(b_hbm, bb.at[gy], lsem.at[1])
    load_a.start()
    load_b.start()
    pl.semaphore_wait(barrier, len(partners))

    made = []

    def remote(src, dst, dev):
        k = len(made)
        copy = pltpu.make_async_remote_copy(
            src_ref=src,
            dst_ref=dst,
            send_sem=ss.at[k],
            recv_sem=rs.at[k],
            device_id=dev,
            device_id_type=MESH,
        )
        made.append(copy)
        return copy

    def tokens(q, size):
        return pl.ds(q * size, size)

    far_q = {q: remote(b_hbm.at[tokens(q, CHK)], bb.at[gy, tokens(q, CHK)], far) for q in range(4)}
    own_r = {h: remote(b_hbm.at[tokens(h, HALF)], bb.at[gy, tokens(h, HALF)], right) for h in range(2)}
    own_l = {h: remote(b_hbm.at[tokens(h, HALF)], bb.at[gy, tokens(h, HALF)], left) for h in range(2)}

    def relay(slot, q, size, dev):
        return remote(bb.at[slot, tokens(q, size)], bb.at[slot, tokens(q, size)], dev)

    hop_r = relay(xl * 2 + zh, 0, HALF, right)
    hop_l = relay(xr * 2 + zh, 1, HALF, left)
    oz = 1 - zh
    far_r = {q: relay(x * 2 + oz, q, CHK, right) for q in range(4)}
    far_l = {q: relay(x * 2 + oz, q, CHK, left) for q in range(4)}
    fhop_r = {q: relay(xl * 2 + oz, q, CHK, right) for q in (0, 1)}
    fhop_l = {q: relay(xr * 2 + oz, q, CHK, left) for q in (2, 3)}

    def rows(block, h=None):
        if h is None:
            return pl.ds(pl.multiple_of(block * BLK, BLK), BLK)
        return pl.ds(pl.multiple_of(block * BLK + h * (BLK // 2), BLK // 2), BLK // 2)

    def pass_on(block, h, dev):
        return remote(at.at[rows(block, h)], at.at[rows(block, h)], dev)

    a_up = {h: pass_on(gz, h, up) for h in range(2)}
    a_down = {h: pass_on(gz, h, down) for h in range(2)}
    ahop_up = pass_on(yl * 2 + c, 0, up)
    ahop_down = pass_on(yr * 2 + c, 1, down)
    sib = {d: pass_on(((y + d) % 4) * 2 + c, None, sibling) for d in range(4)}

    for q in (0, 2, 1, 3):
        far_q[q].start()
    own_r[0].start()
    own_l[1].start()
    own_r[1].start()
    own_l[0].start()

    load_a.wait()

    def turn(k, carry):
        lanes = lax.broadcasted_iota(jnp.int32, (BLK, BLK), 1) + (k % (SEQ // BLK)) * BLK
        kept = lanes < vc[k // (SEQ // BLK)]
        span = pl.ds(pl.multiple_of(k * BLK, BLK), BLK)
        tile = raw[span, :].T
        at[rows(gz), span] = jnp.where(kept, tile, jnp.zeros((), tile.dtype))
        return carry

    lax.fori_loop(0, TOK // BLK, turn, 0)
    a_up[0].start()
    a_down[1].start()
    a_up[1].start()
    a_down[0].start()
    sib[0].start()

    own_r[0].wait_recv()
    hop_r.start()
    own_l[1].wait_recv()
    hop_l.start()
    far_q[0].wait_recv()
    far_r[0].start()
    far_l[0].start()
    a_up[0].wait_recv()
    ahop_up.start()
    a_down[1].wait_recv()
    ahop_down.start()
    far_q[2].wait_recv()
    far_r[2].start()
    far_l[2].start()
    a_up[1].wait_recv()
    sib[3].start()
    a_down[0].wait_recv()
    sib[1].start()
    far_q[1].wait_recv()
    far_r[1].start()
    far_l[1].start()
    ahop_up.wait_recv()
    ahop_down.wait_recv()
    sib[2].start()
    for d in range(4):
        sib[d].wait_recv()

    sends = {}
    for n in range(4):
        for d in range(3):
            sends[n, d] = (
                remote(sbuf.at[d, n], rbuf.at[d, n], owners[d]),
                remote(ssc.at[d, n], rsc.at[d, n], owners[d]),
            )

    def columns(slot):
        return pl.ds(pl.multiple_of(slot * BLK, BLK), BLK)

    def product(d, first, second):
        lhs = at[pl.ds(pl.multiple_of(((zl + d) % 4) * 2 * BLK, 2 * BLK), 2 * BLK), :]
        rhs = jnp.concatenate([bb[first], bb[second]], axis=1)
        return jnp.dot(lhs, rhs, preferred_element_type=jnp.float32)

    def pair(n, first, second):
        for d in range(3):
            part = product(d + 1, first, second)
            top = jnp.maximum(jnp.max(jnp.abs(part), axis=0, keepdims=True), 2e-34)
            sbuf[d, n] = jnp.round(part * (32767.0 / top)).astype(jnp.int32).astype(jnp.int16)
            ssc[d, n] = top * (1.0 / 32767.0)
            for copy in sends[n, d]:
                copy.start()
        part = product(0, first, second)
        out[:, columns(first)] = part[:, :BLK]
        out[:, columns(second)] = part[:, BLK:]

    def gather(n, first, second):
        for d in range(3):
            for copy in sends[n, d]:
                copy.wait_recv()
            part = rbuf[d, n].astype(jnp.int32).astype(jnp.float32) * rsc[d, n]
            out[:, columns(first)] += part[:, :BLK]
            out[:, columns(second)] += part[:, BLK:]

    near = (gy, xr * 2 + zh)
    nearer = (xl * 2 + zh, xo * 2 + zh)
    distant = (x * 2 + oz, xr * 2 + oz)
    last = (xl * 2 + oz, xo * 2 + oz)

    load_b.wait()
    own_l[0].wait_recv()
    pair(0, *near)
    far_r[0].wait_recv()
    fhop_r[0].start()
    far_l[2].wait_recv()
    fhop_l[2].start()
    far_q[3].wait_recv()
    far_r[3].start()
    far_l[3].start()
    own_r[1].wait_recv()
    hop_r.wait_recv()
    hop_l.wait_recv()
    pair(1, *nearer)
    far_r[1].wait_recv()
    fhop_r[1].start()
    far_l[3].wait_recv()
    fhop_l[3].start()
    far_l[0].wait_recv()
    far_l[1].wait_recv()
    pair(2, *distant)
    far_r[2].wait_recv()
    far_r[3].wait_recv()
    for copy in (fhop_r[0], fhop_r[1], fhop_l[2], fhop_l[3]):
        copy.wait_recv()
    pair(3, *last)
    gather(0, *near)
    gather(1, *nearer)
    gather(2, *distant)
    gather(3, *last)
    for copy in made:
        copy.wait_send()


def shards(attn_out, out_grad, valid_counts):
    any_space = pl.BlockSpec(memory_space=pl.ANY)
    return pl.pallas_call(
        kernel,
        out_shape=jax.ShapeDtypeStruct((2 * BLK, 8 * BLK), jnp.float32),
        in_specs=[pl.BlockSpec(memory_space=pltpu.SMEM), any_space, any_space],
        out_specs=pl.BlockSpec(memory_space=pltpu.VMEM),
        scratch_shapes=[
            pltpu.VMEM((TOK, BLK), jnp.bfloat16),
            pltpu.VMEM((8 * BLK, TOK), jnp.bfloat16),
            pltpu.VMEM((8, TOK, BLK), jnp.bfloat16),
            pltpu.VMEM((3, 4, 2 * BLK, 2 * BLK), jnp.int16),
            pltpu.VMEM((3, 4, 2 * BLK, 2 * BLK), jnp.int16),
            pltpu.VMEM((3, 4, 1, 2 * BLK), jnp.float32),
            pltpu.VMEM((3, 4, 1, 2 * BLK), jnp.float32),
            pltpu.SemaphoreType.DMA((2,)),
            pltpu.SemaphoreType.DMA((COPIES,)),
            pltpu.SemaphoreType.DMA((COPIES,)),
        ],
        compiler_params=pltpu.CompilerParams(
            collective_id=0, has_side_effects=True, vmem_limit_bytes=56 * 1024 * 1024
        ),
        cost_estimate=pl.CostEstimate(
            flops=2 * TOK * 1024 * 1024, bytes_accessed=3 << 20, transcendentals=0
        ),
        name="wgrad",
    )(valid_counts, attn_out, out_grad)


def solution(mesh):
    return jax.shard_map(
        shards,
        mesh=mesh,
        in_specs=(P("gx", ("gy", "gz")), P("gx", ("gz", "gy")), P("gx")),
        out_specs=P(("gy", "gx"), "gz"),
        check_vma=False,
    )
```

```python
import functools

import jax
import jax.numpy as jnp
from jax import lax
from jax.experimental import pallas as pl
from jax.experimental.pallas import tpu as pltpu
from jax.sharding import PartitionSpec as P

MESH = pl.DeviceIdType.MESH
TOK = 4096
SEQ = 1024
BLK = 128
CHK = TOK // 4
HALF = TOK // 2
COPIES = 40


def kernel(vc, a_hbm, b_hbm, out, raw, at, bb, sbuf, rbuf, ssc, rsc, acc, lsem, ss, rs, pss, prs):
    zl = lax.axis_index("gx")
    gy = lax.axis_index("gy")
    gz = lax.axis_index("gz")
    x, zh = gy // 2, gy % 2
    y, c = gz // 2, gz % 2
    xr, xl, xo = (x + 1) % 4, (x + 3) % 4, (x + 2) % 4
    yr, yl, yo = (y + 1) % 4, (y + 3) % 4, (y + 2) % 4

    right, left = (zl, xr * 2 + zh, gz), (zl, xl * 2 + zh, gz)
    far = (zl, x * 2 + (1 - zh), gz)
    up, down = (zl, gy, yr * 2 + c), (zl, gy, yl * 2 + c)
    opposite = (zl, gy, yo * 2 + c)
    sibling = (zl, gy, y * 2 + (1 - c))
    owners = [((zl + d) % 4, gy, gz) for d in range(1, 4)]

    barrier = pltpu.get_barrier_semaphore()
    partners = [right, left, far, up, down, sibling] + owners
    for dev in partners:
        pl.semaphore_signal(barrier, inc=1, device_id=dev, device_id_type=MESH)

    load_a = pltpu.make_async_copy(a_hbm, raw, lsem.at[0])
    load_b = pltpu.make_async_copy(b_hbm, bb.at[gy], lsem.at[1])
    load_a.start()
    load_b.start()
    pl.semaphore_wait(barrier, len(partners))

    made = []

    def remote(src, dst, dev):
        k = len(made)
        copy = pltpu.make_async_remote_copy(
            src_ref=src,
            dst_ref=dst,
            send_sem=ss.at[k],
            recv_sem=rs.at[k],
            device_id=dev,
            device_id_type=MESH,
        )
        made.append(copy)
        return copy

    def tokens(q, size):
        return pl.ds(q * size, size)

    far_q = {q: remote(b_hbm.at[tokens(q, CHK)], bb.at[gy, tokens(q, CHK)], far) for q in range(4)}
    own_r = {h: remote(b_hbm.at[tokens(h, HALF)], bb.at[gy, tokens(h, HALF)], right) for h in range(2)}
    own_l = {h: remote(b_hbm.at[tokens(h, HALF)], bb.at[gy, tokens(h, HALF)], left) for h in range(2)}

    def relay(slot, q, size, dev):
        return remote(bb.at[slot, tokens(q, size)], bb.at[slot, tokens(q, size)], dev)

    hop_r = relay(xl * 2 + zh, 0, HALF, right)
    hop_l = relay(xr * 2 + zh, 1, HALF, left)
    oz = 1 - zh
    far_r = {q: relay(x * 2 + oz, q, CHK, right) for q in range(4)}
    far_l = {q: relay(x * 2 + oz, q, CHK, left) for q in range(4)}
    fhop_r = {q: relay(xl * 2 + oz, q, CHK, right) for q in (0, 1)}
    fhop_l = {q: relay(xr * 2 + oz, q, CHK, left) for q in (2, 3)}

    def rows(block, h=None):
        if h is None:
            return pl.ds(pl.multiple_of(block * BLK, BLK), BLK)
        return pl.ds(pl.multiple_of(block * BLK + h * (BLK // 2), BLK // 2), BLK // 2)

    def pass_on(block, h, dev):
        return remote(at.at[rows(block, h)], at.at[rows(block, h)], dev)

    a_up = {h: pass_on(gz, h, up) for h in range(2)}
    a_down = {h: pass_on(gz, h, down) for h in range(2)}
    ahop_up = pass_on(yl * 2 + c, 0, up)
    ahop_down = pass_on(yr * 2 + c, 1, down)
    sib = {d: pass_on(((y + d) % 4) * 2 + c, None, sibling) for d in range(4)}

    for q in (0, 2, 1, 3):
        far_q[q].start()
    own_r[0].start()
    own_l[1].start()
    own_r[1].start()
    own_l[0].start()

    load_a.wait()

    def turn(k, carry):
        lanes = lax.broadcasted_iota(jnp.int32, (BLK, BLK), 1) + (k % (SEQ // BLK)) * BLK
        kept = lanes < vc[k // (SEQ // BLK)]
        span = pl.ds(pl.multiple_of(k * BLK, BLK), BLK)
        tile = raw[span, :].T
        at[rows(gz), span] = jnp.where(kept, tile, jnp.zeros((), tile.dtype))
        return carry

    lax.fori_loop(0, TOK // BLK, turn, 0)
    a_up[0].start()
    a_down[1].start()
    a_up[1].start()
    a_down[0].start()
    sib[0].start()

    own_r[0].wait_recv()
    hop_r.start()
    own_l[1].wait_recv()
    hop_l.start()
    far_q[0].wait_recv()
    far_r[0].start()
    far_l[0].start()
    a_up[0].wait_recv()
    ahop_up.start()
    a_down[1].wait_recv()
    ahop_down.start()
    far_q[2].wait_recv()
    far_r[2].start()
    far_l[2].start()
    a_up[1].wait_recv()
    sib[3].start()
    a_down[0].wait_recv()
    sib[1].start()
    far_q[1].wait_recv()
    far_r[1].start()
    far_l[1].start()
    ahop_up.wait_recv()
    ahop_down.wait_recv()
    sib[2].start()
    for d in range(4):
        sib[d].wait_recv()

    side = zl // 2
    mid = (zl + side) % 2
    end_at, mid_at, far_mid, far_end = 3 * side, 1 + side, 2 - side, 3 - 3 * side
    goal = [
        mid * far_mid + (1 - mid) * far_end,
        mid * end_at + (1 - mid) * far_mid,
        mid * far_end + (1 - mid) * mid_at,
    ]
    goes_to = [
        mid * far_mid + (1 - mid) * mid_at,
        mid * end_at + (1 - mid) * far_mid,
        mid * far_end + (1 - mid) * mid_at,
    ]
    lands = [3 * (1 - mid), 1 - mid, 2 - mid]

    blocks = [gy, xr * 2 + zh, xl * 2 + zh, xo * 2 + zh, x * 2 + oz, xr * 2 + oz, xl * 2 + oz, xo * 2 + oz]
    units = [(0, 2), (2, 2), (4, 2), (6, 1), (7, 1)]

    def part_copies(k, u, slot):
        first, count = units[u]
        span = pl.ds(first, count)
        dev = (goes_to[k], gy, gz)
        return [
            pltpu.make_async_remote_copy(
                src_ref=src.at[k, span],
                dst_ref=dst.at[slot, span],
                send_sem=pss.at[k, u, w],
                recv_sem=prs.at[slot, u, w],
                device_id=dev,
                device_id_type=MESH,
            )
            for w, (src, dst) in enumerate(((sbuf, rbuf), (ssc, rsc)))
        ]

    def columns(slot):
        return pl.ds(pl.multiple_of(slot * BLK, BLK), BLK)

    def product(chunk, u):
        first, count = units[u]
        lhs = at[pl.ds(pl.multiple_of(chunk * 2 * BLK, 2 * BLK), 2 * BLK), :]
        rhs = [bb[blocks[first + i]] for i in range(count)]
        rhs = rhs[0] if count == 1 else jnp.concatenate(rhs, axis=1)
        part = jnp.dot(lhs, rhs, preferred_element_type=jnp.float32)
        return [part[:, i * BLK : (i + 1) * BLK] for i in range(count)]

    def send(k, u, parts):
        first, count = units[u]
        for i in range(count):
            top = jnp.maximum(jnp.max(jnp.abs(parts[i]), axis=0, keepdims=True), 2e-34)
            sbuf[k, first + i] = jnp.round(parts[i] * (32767.0 / top)).astype(jnp.int32).astype(jnp.int16)
            ssc[k, first + i] = top * (1.0 / 32767.0)
        for copy in part_copies(k, u, lands[k]):
            copy.start()

    def arrived(slot, u):
        first, count = units[u]
        for copy in part_copies(0, u, slot):
            copy.wait_recv()
        return [
            rbuf[slot, first + i].astype(jnp.int32).astype(jnp.float32) * rsc[slot, first + i]
            for i in range(count)
        ]

    def unit(u):
        first, count = units[u]
        for k in (0, 1):
            send(k, u, product(goal[k], u))
        parts = product(goal[2], u)

        @pl.when(mid == 0)
        def _():
            send(2, u, parts)

        @pl.when(mid == 1)
        def _():
            for i in range(count):
                acc[first + i] = parts[i]

        parts = product(zl, u)
        for i in range(count):
            out[:, columns(blocks[first + i])] = parts[i]

    def finish(u):
        @pl.when(mid == 1)
        def _():
            first, count = units[u]
            parts = arrived(3, u)
            send(2, u, [acc[first + i] + parts[i] for i in range(count)])

    def gather(u):
        first, count = units[u]

        def add(slot):
            parts = arrived(slot, u)
            for i in range(count):
                out[:, columns(blocks[first + i])] += parts[i]

        add(0)

        @pl.when(mid == 1)
        def _():
            add(2)

        add(1)

    load_b.wait()
    own_l[0].wait_recv()
    unit(0)
    far_r[0].wait_recv()
    fhop_r[0].start()
    far_l[2].wait_recv()
    fhop_l[2].start()
    far_q[3].wait_recv()
    far_r[3].start()
    far_l[3].start()
    own_r[1].wait_recv()
    hop_r.wait_recv()
    hop_l.wait_recv()
    unit(1)
    far_r[1].wait_recv()
    fhop_r[1].start()
    far_l[3].wait_recv()
    fhop_l[3].start()
    finish(0)
    far_l[0].wait_recv()
    far_l[1].wait_recv()
    unit(2)
    finish(1)
    far_r[2].wait_recv()
    far_r[3].wait_recv()
    unit(3)
    finish(2)
    gather(0)
    for copy in (fhop_r[0], fhop_r[1], fhop_l[2], fhop_l[3]):
        copy.wait_recv()
    unit(4)
    finish(3)
    gather(1)
    finish(4)
    for u in (2, 3, 4):
        gather(u)
    for copy in made:
        copy.wait_send()
    for u in range(5):
        for k in range(3):
            for copy in part_copies(k, u, 0):
                copy.wait_send()


def shards(attn_out, out_grad, valid_counts):
    any_space = pl.BlockSpec(memory_space=pl.ANY)
    return pl.pallas_call(
        kernel,
        out_shape=jax.ShapeDtypeStruct((2 * BLK, 8 * BLK), jnp.float32),
        in_specs=[pl.BlockSpec(memory_space=pltpu.SMEM), any_space, any_space],
        out_specs=pl.BlockSpec(memory_space=pltpu.VMEM),
        scratch_shapes=[
            pltpu.VMEM((TOK, BLK), jnp.bfloat16),
            pltpu.VMEM((8 * BLK, TOK), jnp.bfloat16),
            pltpu.VMEM((8, TOK, BLK), jnp.bfloat16),
            pltpu.VMEM((3, 8, 2 * BLK, BLK), jnp.int16),
            pltpu.VMEM((4, 8, 2 * BLK, BLK), jnp.int16),
            pltpu.VMEM((3, 8, 1, BLK), jnp.float32),
            pltpu.VMEM((4, 8, 1, BLK), jnp.float32),
            pltpu.VMEM((8, 2 * BLK, BLK), jnp.float32),
            pltpu.SemaphoreType.DMA((2,)),
            pltpu.SemaphoreType.DMA((COPIES,)),
            pltpu.SemaphoreType.DMA((COPIES,)),
            pltpu.SemaphoreType.DMA((3, 5, 2)),
            pltpu.SemaphoreType.DMA((4, 5, 2)),
        ],
        compiler_params=pltpu.CompilerParams(
            collective_id=0, has_side_effects=True, vmem_limit_bytes=56 * 1024 * 1024
        ),
        cost_estimate=pl.CostEstimate(
            flops=2 * TOK * 1024 * 1024, bytes_accessed=3 << 20, transcendentals=0
        ),
        name="wgrad",
    )(valid_counts, attn_out, out_grad)


def solution(mesh):
    return jax.shard_map(
        shards,
        mesh=mesh,
        in_specs=(P("gx", ("gy", "gz")), P("gx", ("gz", "gy")), P("gx")),
        out_specs=P(("gy", "gx"), "gz"),
        check_vma=False,
    )
```

```python
import functools

import jax
import jax.numpy as jnp
from jax import lax
from jax.experimental import pallas as pl
from jax.experimental.pallas import tpu as pltpu
from jax.sharding import PartitionSpec as P

MESH = pl.DeviceIdType.MESH
TOK = 4096
SEQ = 1024
BLK = 128
GRAIN = 32
CAPS = (2304, 2560, 2816, 3072, 3328, 3584, 4096)
COPIES = 40


def compact(vc, a_hbm, b_hbm, at_out, b_out, which, raw_a, raw_b, mine, theirs, lsem, ss, rs):
    zl = lax.axis_index("gx")
    gy = lax.axis_index("gy")
    gz = lax.axis_index("gz")
    barrier = pltpu.get_barrier_semaphore()
    peers = [((zl + d) % 4, gy, gz) for d in range(1, 4)]
    for dev in peers:
        pl.semaphore_signal(barrier, inc=1, device_id=dev, device_id_type=MESH)
    load_a = pltpu.make_async_copy(a_hbm, raw_a, lsem.at[0])
    load_b = pltpu.make_async_copy(b_hbm, raw_b, lsem.at[1])
    load_a.start()
    load_b.start()

    rows_here = TOK // SEQ
    valid = [vc[r] for r in range(rows_here)]
    first = [0]
    for r in range(rows_here):
        first.append(first[-1] + (valid[r] + GRAIN - 1) // GRAIN)
    mine[...] = jnp.full(mine.shape, first[-1] * GRAIN, jnp.int32)
    pl.semaphore_wait(barrier, len(peers))
    copies = [
        pltpu.make_async_remote_copy(
            src_ref=mine, dst_ref=theirs.at[d], send_sem=ss.at[d], recv_sem=rs.at[d],
            device_id=peers[d], device_id_type=MESH,
        )
        for d in range(3)
    ]
    for copy in copies:
        copy.start()
    load_a.wait()
    load_b.wait()

    def tile(k, carry):
        pieces = []
        for i in range(BLK // GRAIN):
            n = k * (BLK // GRAIN) + i
            begin, row, count = first[0], 0, valid[0]
            for r in range(1, rows_here):
                past = n >= first[r]
                begin = jnp.where(past, first[r], begin)
                row = jnp.where(past, r, row)
                count = jnp.where(past, valid[r], count)
            slot = (n - begin) * GRAIN
            source = jnp.minimum(row * (SEQ // GRAIN) + n - begin, TOK // GRAIN - 1)
            kept = lax.broadcasted_iota(jnp.int32, (GRAIN, BLK), 0) + slot < count
            piece = raw_a[source]
            pieces.append(jnp.where(kept, piece, jnp.zeros((), piece.dtype)))
            b_out[pl.ds(pl.multiple_of(n * GRAIN, GRAIN), GRAIN), :] = raw_b[source]
        span = pl.ds(pl.multiple_of(k * BLK, BLK), BLK)
        at_out[:, span] = jnp.concatenate(pieces, axis=0).T
        return carry

    lax.fori_loop(0, TOK // BLK, tile, 0)
    for copy in copies:
        copy.wait_recv()
    most = jnp.maximum(jnp.maximum(mine[...], theirs[0]), jnp.maximum(theirs[1], theirs[2]))
    which[...] = sum(jnp.where(most > cap, 1, 0) for cap in CAPS[:-1])
    for copy in copies:
        copy.wait_send()


def kernel(cap, a_hbm, b_hbm, out, at, bb, sbuf, rbuf, ssc, rsc, acc, lsem, ss, rs, pss, prs):
    CHK, HALF = cap // 4, cap // 2
    zl = lax.axis_index("gx")
    gy = lax.axis_index("gy")
    gz = lax.axis_index("gz")
    x, zh = gy // 2, gy % 2
    y, c = gz // 2, gz % 2
    xr, xl, xo = (x + 1) % 4, (x + 3) % 4, (x + 2) % 4
    yr, yl, yo = (y + 1) % 4, (y + 3) % 4, (y + 2) % 4

    right, left = (zl, xr * 2 + zh, gz), (zl, xl * 2 + zh, gz)
    far = (zl, x * 2 + (1 - zh), gz)
    up, down = (zl, gy, yr * 2 + c), (zl, gy, yl * 2 + c)
    sibling = (zl, gy, y * 2 + (1 - c))
    owners = [((zl + d) % 4, gy, gz) for d in range(1, 4)]

    barrier = pltpu.get_barrier_semaphore()
    partners = [right, left, far, up, down, sibling] + owners
    for dev in partners:
        pl.semaphore_signal(barrier, inc=1, device_id=dev, device_id_type=MESH)

    def rows(block, h=None):
        if h is None:
            return pl.ds(pl.multiple_of(block * BLK, BLK), BLK)
        return pl.ds(pl.multiple_of(block * BLK + h * (BLK // 2), BLK // 2), BLK // 2)

    load_a = pltpu.make_async_copy(a_hbm.at[:, pl.ds(0, cap)], at.at[rows(gz)], lsem.at[0])
    load_b = pltpu.make_async_copy(b_hbm.at[pl.ds(0, cap)], bb.at[gy], lsem.at[1])
    load_a.start()
    load_b.start()
    pl.semaphore_wait(barrier, len(partners))

    made = []

    def remote(src, dst, dev):
        k = len(made)
        copy = pltpu.make_async_remote_copy(
            src_ref=src,
            dst_ref=dst,
            send_sem=ss.at[k],
            recv_sem=rs.at[k],
            device_id=dev,
            device_id_type=MESH,
        )
        made.append(copy)
        return copy

    def tokens(q, size):
        return pl.ds(q * size, size)

    far_q = {q: remote(b_hbm.at[tokens(q, CHK)], bb.at[gy, tokens(q, CHK)], far) for q in range(4)}
    own_r = {h: remote(b_hbm.at[tokens(h, HALF)], bb.at[gy, tokens(h, HALF)], right) for h in range(2)}
    own_l = {h: remote(b_hbm.at[tokens(h, HALF)], bb.at[gy, tokens(h, HALF)], left) for h in range(2)}

    def relay(slot, q, size, dev):
        return remote(bb.at[slot, tokens(q, size)], bb.at[slot, tokens(q, size)], dev)

    hop_r = relay(xl * 2 + zh, 0, HALF, right)
    hop_l = relay(xr * 2 + zh, 1, HALF, left)
    oz = 1 - zh
    far_r = {q: relay(x * 2 + oz, q, CHK, right) for q in range(4)}
    far_l = {q: relay(x * 2 + oz, q, CHK, left) for q in range(4)}
    fhop_r = {q: relay(xl * 2 + oz, q, CHK, right) for q in (0, 1)}
    fhop_l = {q: relay(xr * 2 + oz, q, CHK, left) for q in (2, 3)}

    def pass_on(block, h, dev):
        return remote(at.at[rows(block, h)], at.at[rows(block, h)], dev)

    def own(h, dev):
        part = pl.ds(h * (BLK // 2), BLK // 2)
        return remote(a_hbm.at[part, pl.ds(0, cap)], at.at[rows(gz, h)], dev)

    a_up = {h: own(h, up) for h in range(2)}
    a_down = {h: own(h, down) for h in range(2)}
    ahop_up = pass_on(yl * 2 + c, 0, up)
    ahop_down = pass_on(yr * 2 + c, 1, down)
    sib = {d: pass_on(((y + d) % 4) * 2 + c, None, sibling) for d in range(1, 4)}
    sib[0] = remote(a_hbm.at[:, pl.ds(0, cap)], at.at[rows(gz)], sibling)

    for q in (0, 2, 1, 3):
        far_q[q].start()
    own_r[0].start()
    own_l[1].start()
    own_r[1].start()
    own_l[0].start()

    a_up[0].start()
    a_down[1].start()
    a_up[1].start()
    a_down[0].start()
    sib[0].start()

    own_r[0].wait_recv()
    hop_r.start()
    own_l[1].wait_recv()
    hop_l.start()
    a_up[0].wait_recv()
    ahop_up.start()
    a_down[1].wait_recv()
    ahop_down.start()
    far_q[0].wait_recv()
    far_r[0].start()
    far_l[0].start()
    a_up[1].wait_recv()
    sib[3].start()
    a_down[0].wait_recv()
    sib[1].start()
    far_q[2].wait_recv()
    far_r[2].start()
    far_l[2].start()
    ahop_up.wait_recv()
    ahop_down.wait_recv()
    sib[2].start()
    far_q[1].wait_recv()
    far_r[1].start()
    far_l[1].start()
    for d in range(4):
        sib[d].wait_recv()

    side = zl // 2
    mid = (zl + side) % 2
    end_at, mid_at, far_mid, far_end = 3 * side, 1 + side, 2 - side, 3 - 3 * side
    goal = [
        mid * far_mid + (1 - mid) * far_end,
        mid * end_at + (1 - mid) * far_mid,
        mid * far_end + (1 - mid) * mid_at,
    ]
    goes_to = [
        mid * far_mid + (1 - mid) * mid_at,
        mid * end_at + (1 - mid) * far_mid,
        mid * far_end + (1 - mid) * mid_at,
    ]
    lands = [3 * (1 - mid), 1 - mid, 2 - mid]

    blocks = [gy, xr * 2 + zh, xl * 2 + zh, xo * 2 + zh, x * 2 + oz, xr * 2 + oz, xl * 2 + oz, xo * 2 + oz]
    units = [(0, 2), (2, 2), (4, 2), (6, 1), (7, 1)]

    def pick(choices, k):
        if isinstance(k, int):
            return choices[k]
        value = choices[-1]
        for i in range(len(choices) - 1):
            value = jnp.where(k == i, choices[i], value)
        return value

    def part_copies(k, u, slot):
        first, count = units[u]
        span = pl.ds(first, count)
        dev = (pick(goes_to, k), gy, gz)
        return [
            pltpu.make_async_remote_copy(
                src_ref=src.at[k, span],
                dst_ref=dst.at[slot, span],
                send_sem=pss.at[k, u, w],
                recv_sem=prs.at[slot, u, w],
                device_id=dev,
                device_id_type=MESH,
            )
            for w, (src, dst) in enumerate(((sbuf, rbuf), (ssc, rsc)))
        ]

    def columns(slot):
        return pl.ds(pl.multiple_of(slot * BLK, BLK), BLK)

    def product(chunk, u):
        first, count = units[u]
        lhs = at[pl.ds(pl.multiple_of(chunk * 2 * BLK, 2 * BLK), 2 * BLK), :]
        rhs = [bb[blocks[first + i]] for i in range(count)]
        rhs = rhs[0] if count == 1 else jnp.concatenate(rhs, axis=1)
        part = jnp.dot(lhs, rhs, preferred_element_type=jnp.float32)
        return [part[:, i * BLK : (i + 1) * BLK] for i in range(count)]

    def send(k, u, parts):
        first, count = units[u]
        for i in range(count):
            top = jnp.maximum(jnp.max(jnp.abs(parts[i]), axis=0, keepdims=True), 2e-34)
            sbuf[k, first + i] = jnp.round(parts[i] * (32767.0 / top)).astype(jnp.int32).astype(jnp.int16)
            ssc[k, first + i] = top * (1.0 / 32767.0)
        for copy in part_copies(k, u, pick(lands, k)):
            copy.start()

    def arrived(slot, u):
        first, count = units[u]
        for copy in part_copies(0, u, slot):
            copy.wait_recv()
        return [
            rbuf[slot, first + i].astype(jnp.int32).astype(jnp.float32) * rsc[slot, first + i]
            for i in range(count)
        ]

    def unit(u):
        first, count = units[u]

        def step(k, carry):
            parts = product(pick(goal + [zl], k), u)
            held = jnp.logical_and(k == 2, mid == 1)

            @pl.when(jnp.logical_and(k < 3, jnp.logical_not(held)))
            def _():
                send(k, u, parts)

            @pl.when(held)
            def _():
                for i in range(count):
                    acc[first + i] = parts[i]

            @pl.when(k == 3)
            def _():
                for i in range(count):
                    out[:, columns(blocks[first + i])] = parts[i]

            return carry

        lax.fori_loop(0, 4, step, 0)

    def finish(u):
        @pl.when(mid == 1)
        def _():
            first, count = units[u]
            parts = arrived(3, u)
            send(2, u, [acc[first + i] + parts[i] for i in range(count)])

    def gather(u):
        first, count = units[u]

        def add(slot):
            parts = arrived(slot, u)
            for i in range(count):
                out[:, columns(blocks[first + i])] += parts[i]

        add(0)

        @pl.when(mid == 1)
        def _():
            add(2)

        add(1)

    load_a.wait()
    load_b.wait()
    own_l[0].wait_recv()
    unit(0)
    far_q[3].wait_recv()
    far_r[3].start()
    far_l[3].start()
    far_r[0].wait_recv()
    fhop_r[0].start()
    far_l[2].wait_recv()
    fhop_l[2].start()
    own_r[1].wait_recv()
    hop_r.wait_recv()
    hop_l.wait_recv()
    unit(1)
    far_r[1].wait_recv()
    fhop_r[1].start()
    far_l[3].wait_recv()
    fhop_l[3].start()
    far_l[0].wait_recv()
    far_l[1].wait_recv()
    finish(0)
    unit(2)
    finish(1)
    far_r[2].wait_recv()
    far_r[3].wait_recv()
    unit(3)
    finish(2)
    gather(0)
    fhop_r[0].wait_recv()
    fhop_r[1].wait_recv()
    fhop_l[2].wait_recv()
    fhop_l[3].wait_recv()
    unit(4)
    finish(3)
    gather(1)
    finish(4)
    gather(2)
    gather(3)
    gather(4)
    for copy in made:
        copy.wait_send()
    for u in range(5):
        for k in range(3):
            for copy in part_copies(k, u, 0):
                copy.wait_send()


def main(cap, number):
    any_space = pl.BlockSpec(memory_space=pl.ANY)
    return pl.pallas_call(
        functools.partial(kernel, cap),
        out_shape=jax.ShapeDtypeStruct((2 * BLK, 8 * BLK), jnp.float32),
        in_specs=[any_space, any_space],
        out_specs=pl.BlockSpec(memory_space=pltpu.VMEM),
        scratch_shapes=[
            pltpu.VMEM((8 * BLK, cap), jnp.bfloat16),
            pltpu.VMEM((8, cap, BLK), jnp.bfloat16),
            pltpu.VMEM((3, 8, 2 * BLK, BLK), jnp.int16),
            pltpu.VMEM((4, 8, 2 * BLK, BLK), jnp.int16),
            pltpu.VMEM((3, 8, 1, BLK), jnp.float32),
            pltpu.VMEM((4, 8, 1, BLK), jnp.float32),
            pltpu.VMEM((8, 2 * BLK, BLK), jnp.float32),
            pltpu.SemaphoreType.DMA((2,)),
            pltpu.SemaphoreType.DMA((COPIES,)),
            pltpu.SemaphoreType.DMA((COPIES,)),
            pltpu.SemaphoreType.DMA((3, 5, 2)),
            pltpu.SemaphoreType.DMA((4, 5, 2)),
        ],
        compiler_params=pltpu.CompilerParams(
            collective_id=number, has_side_effects=True, vmem_limit_bytes=48 * 1024 * 1024
        ),
        cost_estimate=pl.CostEstimate(
            flops=2 * cap * 1024 * 1024, bytes_accessed=3 << 20, transcendentals=0
        ),
        name=f"wgrad{cap}",
    )


def shards(attn_out, out_grad, valid_counts):
    hbm = pl.BlockSpec(memory_space=pltpu.HBM)
    vmem = pl.BlockSpec(memory_space=pltpu.VMEM)
    grains = [value.reshape(TOK // GRAIN, GRAIN, BLK) for value in (attn_out, out_grad)]
    turned, packed, which = pl.pallas_call(
        compact,
        out_shape=(
            jax.ShapeDtypeStruct((BLK, TOK), attn_out.dtype),
            jax.ShapeDtypeStruct((TOK, BLK), out_grad.dtype),
            jax.ShapeDtypeStruct((8, BLK), jnp.int32),
        ),
        in_specs=[pl.BlockSpec(memory_space=pltpu.SMEM), hbm, hbm],
        out_specs=(vmem, vmem, vmem),
        scratch_shapes=[
            pltpu.VMEM((TOK // GRAIN, GRAIN, BLK), jnp.bfloat16),
            pltpu.VMEM((TOK // GRAIN, GRAIN, BLK), jnp.bfloat16),
            pltpu.VMEM((8, BLK), jnp.int32),
            pltpu.VMEM((3, 8, BLK), jnp.int32),
            pltpu.SemaphoreType.DMA((3,)),
            pltpu.SemaphoreType.DMA((3,)),
            pltpu.SemaphoreType.DMA((3,)),
        ],
        compiler_params=pltpu.CompilerParams(
            collective_id=0, has_side_effects=True, vmem_limit_bytes=16 * 1024 * 1024
        ),
        name="compact",
    )(valid_counts, *(pltpu.with_memory_space_constraint(value, pltpu.HBM) for value in grains))
    branches = [main(cap, 1 + i) for i, cap in enumerate(CAPS)]
    return lax.switch(which[0, 0], branches, turned, packed)


def solution(mesh):
    return jax.shard_map(
        shards,
        mesh=mesh,
        in_specs=(P("gx", ("gy", "gz")), P("gx", ("gz", "gy")), P("gx")),
        out_specs=P(("gy", "gx"), "gz"),
        check_vma=False,
    )
```

```python
import functools

import jax
import jax.numpy as jnp
from jax import lax
from jax.experimental import pallas as pl
from jax.experimental.pallas import tpu as pltpu
from jax.sharding import PartitionSpec as P

MESH = pl.DeviceIdType.MESH
TOK = 4096
SEQ = 1024
BLK = 128
GRAIN = 32
CAPS = (2432, 2560, 2688, 2816, 2944, 3072, 3200, 3328, 3584, 4096)
UNROLL = 4
COPIES = 32


def compact(vc_hbm, a_hbm, b_hbm, at_out, b_out, which, vc, raw_a, raw_b, mine, theirs, csem, lsem, ss, rs):
    zl = lax.axis_index("gx")
    gy = lax.axis_index("gy")
    gz = lax.axis_index("gz")
    rows_here = TOK // SEQ
    barrier = pltpu.get_barrier_semaphore()
    peers = [((zl + d) % 4, gy, gz) for d in range(1, 4)]
    for dev in peers:
        pl.semaphore_signal(barrier, inc=1, device_id=dev, device_id_type=MESH)
    counts = pltpu.make_async_copy(vc_hbm, vc, csem)
    counts.start()
    loads = []
    for r in range(rows_here):
        part = pl.ds(r * (SEQ // GRAIN), SEQ // GRAIN)
        loads.append(pltpu.make_async_copy(a_hbm.at[part], raw_a.at[part], lsem.at[0, r]))
        loads.append(pltpu.make_async_copy(b_hbm.at[part], raw_b.at[part], lsem.at[1, r]))
    for load in loads:
        load.start()
    counts.wait()
    valid = [vc[r] for r in range(rows_here)]
    first = [0]
    for r in range(rows_here):
        first.append(first[-1] + (valid[r] + GRAIN - 1) // GRAIN)
    mine[...] = jnp.full(mine.shape, first[-1] * GRAIN, jnp.int32)
    pl.semaphore_wait(barrier, len(peers))
    copies = [
        pltpu.make_async_remote_copy(
            src_ref=mine, dst_ref=theirs.at[d], send_sem=ss.at[d], recv_sem=rs.at[d],
            device_id=peers[d], device_id_type=MESH,
        )
        for d in range(3)
    ]
    for copy in copies:
        copy.start()
    for load in loads:
        load.wait()

    def tile(k):
        pieces = []
        for i in range(BLK // GRAIN):
            n = k * (BLK // GRAIN) + i
            begin, row, count = first[0], 0, valid[0]
            for r in range(1, rows_here):
                past = n >= first[r]
                begin = jnp.where(past, first[r], begin)
                row = jnp.where(past, r, row)
                count = jnp.where(past, valid[r], count)
            slot = n - begin
            source = jnp.minimum(row * (SEQ // GRAIN) + slot, TOK // GRAIN - 1)
            kept = lax.broadcasted_iota(jnp.int32, (GRAIN, BLK), 0) + slot * GRAIN < count
            piece = raw_a[source]
            pieces.append(jnp.where(kept, piece, jnp.zeros((), piece.dtype)))
            b_out[pl.ds(pl.multiple_of(n * GRAIN, GRAIN), GRAIN), :] = raw_b[source]
        span = pl.ds(pl.multiple_of(k * BLK, BLK), BLK)
        at_out[:, span] = jnp.concatenate(pieces, axis=0).T

    def tiles(k, carry):
        for i in range(UNROLL):
            tile(k * UNROLL + i)
        return carry

    lax.fori_loop(0, TOK // BLK // UNROLL, tiles, 0)
    for copy in copies:
        copy.wait_recv()
    most = first[-1] * GRAIN
    for d in range(3):
        most = jnp.maximum(most, theirs[d, 0, 0])
    index = 0
    for cap in CAPS[:-1]:
        index = index + jnp.where(most > cap, 1, 0)
    which[0] = index
    for copy in copies:
        copy.wait_send()


def kernel(cap, a_hbm, b_hbm, result, out, at, bb, sbuf, rbuf, ssc, rsc, acc, lsem, osem, sent, rs, prs):
    CHK, HALF = cap // 4, cap // 2
    zl = lax.axis_index("gx")
    gy = lax.axis_index("gy")
    gz = lax.axis_index("gz")
    x, zh = gy // 2, gy % 2
    y, c = gz // 2, gz % 2
    xr, xl, xo = (x + 1) % 4, (x + 3) % 4, (x + 2) % 4
    yr, yl, yo = (y + 1) % 4, (y + 3) % 4, (y + 2) % 4

    right, left = (zl, xr * 2 + zh, gz), (zl, xl * 2 + zh, gz)
    far = (zl, x * 2 + (1 - zh), gz)
    up, down = (zl, gy, yr * 2 + c), (zl, gy, yl * 2 + c)
    sibling = (zl, gy, y * 2 + (1 - c))
    owners = [((zl + d) % 4, gy, gz) for d in range(1, 4)]

    barrier = pltpu.get_barrier_semaphore()
    partners = [right, left, far, up, down, sibling] + owners
    for dev in partners:
        pl.semaphore_signal(barrier, inc=1, device_id=dev, device_id_type=MESH)

    def rows(block, h=None):
        if h is None:
            return pl.ds(pl.multiple_of(block * BLK, BLK), BLK)
        return pl.ds(pl.multiple_of(block * BLK + h * (BLK // 2), BLK // 2), BLK // 2)

    load_a = pltpu.make_async_copy(a_hbm.at[:, pl.ds(0, cap)], at.at[rows(gz)], lsem.at[0])
    load_b = pltpu.make_async_copy(b_hbm.at[pl.ds(0, cap)], bb.at[gy], lsem.at[1])
    load_a.start()
    load_b.start()
    pl.semaphore_wait(barrier, len(partners))

    made = []

    def remote(src, dst, dev, kind=0):
        k = len(made)
        copy = pltpu.make_async_remote_copy(
            src_ref=src,
            dst_ref=dst,
            send_sem=sent.at[kind],
            recv_sem=rs.at[k],
            device_id=dev,
            device_id_type=MESH,
        )
        made.append(copy)
        return copy

    def tokens(q, size):
        return pl.ds(q * size, size)

    far_q = {q: remote(b_hbm.at[tokens(q, CHK)], bb.at[gy, tokens(q, CHK)], far) for q in range(4)}
    own_r = {h: remote(b_hbm.at[tokens(h, HALF)], bb.at[gy, tokens(h, HALF)], right) for h in range(2)}
    own_l = {h: remote(b_hbm.at[tokens(h, HALF)], bb.at[gy, tokens(h, HALF)], left) for h in range(2)}

    def relay(slot, q, size, dev):
        return remote(bb.at[slot, tokens(q, size)], bb.at[slot, tokens(q, size)], dev)

    hop_r = relay(xl * 2 + zh, 0, HALF, right)
    hop_l = relay(xr * 2 + zh, 1, HALF, left)
    oz = 1 - zh
    far_r = {q: relay(x * 2 + oz, q, CHK, right) for q in range(4)}
    far_l = {q: relay(x * 2 + oz, q, CHK, left) for q in range(4)}
    fhop_r = {q: relay(xl * 2 + oz, q, CHK, right) for q in (0, 1)}
    fhop_l = {q: relay(xr * 2 + oz, q, CHK, left) for q in (2, 3)}

    def pass_on(block, h, dev):
        return remote(at.at[rows(block, h)], at.at[rows(block, h)], dev, 1)

    def own(h, dev):
        part = pl.ds(h * (BLK // 2), BLK // 2)
        return remote(a_hbm.at[part, pl.ds(0, cap)], at.at[rows(gz, h)], dev, 1)

    a_up = {h: own(h, up) for h in range(2)}
    a_down = {h: own(h, down) for h in range(2)}
    ahop_up = pass_on(yl * 2 + c, 0, up)
    ahop_down = pass_on(yr * 2 + c, 1, down)
    sib = {d: pass_on(((y + d) % 4) * 2 + c, None, sibling) for d in range(1, 4)}
    sib[0] = remote(a_hbm.at[:, pl.ds(0, cap)], at.at[rows(gz)], sibling, 1)

    for q in (0, 2, 1, 3):
        far_q[q].start()
    own_r[0].start()
    own_l[1].start()
    own_r[1].start()
    own_l[0].start()

    a_up[0].start()
    a_down[1].start()
    a_up[1].start()
    a_down[0].start()
    sib[0].start()

    own_r[0].wait_recv()
    hop_r.start()
    own_l[1].wait_recv()
    hop_l.start()
    a_up[0].wait_recv()
    ahop_up.start()
    a_down[1].wait_recv()
    ahop_down.start()
    far_q[0].wait_recv()
    far_r[0].start()
    far_l[0].start()
    a_up[1].wait_recv()
    sib[3].start()
    a_down[0].wait_recv()
    sib[1].start()
    far_q[2].wait_recv()
    far_r[2].start()
    far_l[2].start()
    ahop_up.wait_recv()
    ahop_down.wait_recv()
    sib[2].start()
    far_q[1].wait_recv()
    far_r[1].start()
    far_l[1].start()
    for d in range(4):
        sib[d].wait_recv()

    side = zl // 2
    mid = (zl + side) % 2
    end_at, mid_at, far_mid, far_end = 3 * side, 1 + side, 2 - side, 3 - 3 * side
    goal = [
        mid * far_mid + (1 - mid) * far_end,
        mid * end_at + (1 - mid) * far_mid,
        mid * far_end + (1 - mid) * mid_at,
    ]
    goes_to = [
        mid * far_mid + (1 - mid) * mid_at,
        mid * end_at + (1 - mid) * far_mid,
        mid * far_end + (1 - mid) * mid_at,
    ]
    lands = [3 * (1 - mid), 1 - mid, 2 - mid]

    blocks = [gy, xr * 2 + zh, xl * 2 + zh, xo * 2 + zh, x * 2 + oz, xr * 2 + oz, xl * 2 + oz, xo * 2 + oz]

    def pick(choices, k):
        if isinstance(k, int):
            return choices[k]
        value = choices[-1]
        for i in range(len(choices) - 1):
            value = jnp.where(k == i, choices[i], value)
        return value

    def part_copies(k, u, slot):
        span = pl.ds(2 * u, 2)
        dev = (pick(goes_to, k), gy, gz)
        return [
            pltpu.make_async_remote_copy(
                src_ref=src.at[k, span],
                dst_ref=dst.at[slot, span],
                send_sem=sent.at[2 + w],
                recv_sem=prs.at[slot, u, w],
                device_id=dev,
                device_id_type=MESH,
            )
            for w, (src, dst) in enumerate(((sbuf, rbuf), (ssc, rsc)))
        ]

    def columns(u, i):
        return pl.ds(pl.multiple_of(pick(blocks[i::2], u) * BLK, BLK), BLK)

    def product(chunk, u):
        lhs = at[pl.ds(pl.multiple_of(chunk * 2 * BLK, 2 * BLK), 2 * BLK), :]
        rhs = jnp.concatenate([bb[pick(blocks[i::2], u)] for i in range(2)], axis=1)
        part = jnp.dot(lhs, rhs, preferred_element_type=jnp.float32)
        return [part[:, :BLK], part[:, BLK:]]

    def send(k, u, parts):
        for i in range(2):
            top = jnp.maximum(jnp.max(jnp.abs(parts[i]), axis=0, keepdims=True), 2e-34)
            sbuf[k, 2 * u + i] = jnp.round(parts[i] * (32767.0 / top)).astype(jnp.int32).astype(jnp.int16)
            ssc[k, 2 * u + i] = top * (1.0 / 32767.0)
        for copy in part_copies(k, u, pick(lands, k)):
            copy.start()

    def arrived(slot, u):
        for copy in part_copies(0, u, slot):
            copy.wait_recv()
        return [
            rbuf[slot, 2 * u + i].astype(jnp.int32).astype(jnp.float32) * rsc[slot, 2 * u + i]
            for i in range(2)
        ]

    def unit(u):
        def step(k, carry):
            parts = product(pick(goal + [zl], k), u)
            held = jnp.logical_and(k == 2, mid == 1)

            @pl.when(jnp.logical_and(k < 3, jnp.logical_not(held)))
            def _():
                send(k, u, parts)

            @pl.when(held)
            def _():
                for i in range(2):
                    acc[2 * u + i] = parts[i]

            @pl.when(k == 3)
            def _():
                for i in range(2):
                    out[:, columns(u, i)] = parts[i]

            return carry

        lax.fori_loop(0, 4, step, 0)

    def finish(u):
        parts = arrived(3, u)
        send(2, u, [acc[2 * u + i] + parts[i] for i in range(2)])

    def stores(u):
        return [
            pltpu.make_async_copy(out.at[:, columns(u, i)], result.at[:, columns(u, i)], osem)
            for i in range(2)
        ]

    def gather(u, carry):
        def add(slot):
            parts = arrived(slot, u)
            for i in range(2):
                out[:, columns(u, i)] += parts[i]

        add(0)

        @pl.when(mid == 1)
        def _():
            add(2)

        add(1)
        for copy in stores(u):
            copy.start()
        return carry

    def stage(u, carry):
        @pl.when(u == 0)
        def _():
            load_a.wait()
            load_b.wait()
            own_l[0].wait_recv()

        @pl.when(u == 1)
        def _():
            far_q[3].wait_recv()
            far_r[3].start()
            far_l[3].start()
            far_r[0].wait_recv()
            fhop_r[0].start()
            far_l[2].wait_recv()
            fhop_l[2].start()
            own_r[1].wait_recv()
            hop_r.wait_recv()
            hop_l.wait_recv()

        @pl.when(u == 2)
        def _():
            far_r[1].wait_recv()
            fhop_r[1].start()
            far_l[3].wait_recv()
            fhop_l[3].start()
            far_l[0].wait_recv()
            far_l[1].wait_recv()

        @pl.when(u == 3)
        def _():
            far_r[2].wait_recv()
            far_r[3].wait_recv()
            fhop_r[0].wait_recv()
            fhop_r[1].wait_recv()
            fhop_l[2].wait_recv()
            fhop_l[3].wait_recv()

        unit(u)

        @pl.when(jnp.logical_and(u > 0, mid == 1))
        def _():
            finish(u - 1)

        return carry

    lax.fori_loop(0, 4, stage, 0)

    @pl.when(mid == 1)
    def _():
        finish(3)

    lax.fori_loop(0, 4, gather, 0)
    pltpu.make_async_copy(out, result, osem).wait()
    pltpu.make_async_copy(bb.at[pl.ds(0, 7)], bb.at[pl.ds(0, 7)], sent.at[0]).wait()
    pltpu.make_async_copy(at.at[pl.ds(0, 7 * BLK)], at.at[pl.ds(0, 7 * BLK)], sent.at[1]).wait()
    pltpu.make_async_copy(sbuf, sbuf, sent.at[2]).wait()
    pltpu.make_async_copy(ssc, ssc, sent.at[3]).wait()


def main(cap, number):
    any_space = pl.BlockSpec(memory_space=pl.ANY)
    return pl.pallas_call(
        functools.partial(kernel, cap),
        out_shape=jax.ShapeDtypeStruct((2 * BLK, 8 * BLK), jnp.float32),
        in_specs=[any_space] * 2,
        out_specs=any_space,
        scratch_shapes=[
            pltpu.VMEM((2 * BLK, 8 * BLK), jnp.float32),
            pltpu.VMEM((8 * BLK, cap), jnp.bfloat16),
            pltpu.VMEM((8, cap, BLK), jnp.bfloat16),
            pltpu.VMEM((3, 8, 2 * BLK, BLK), jnp.int16),
            pltpu.VMEM((4, 8, 2 * BLK, BLK), jnp.int16),
            pltpu.VMEM((3, 8, 1, BLK), jnp.float32),
            pltpu.VMEM((4, 8, 1, BLK), jnp.float32),
            pltpu.VMEM((8, 2 * BLK, BLK), jnp.float32),
            pltpu.SemaphoreType.DMA((2,)),
            pltpu.SemaphoreType.DMA,
            pltpu.SemaphoreType.DMA((4,)),
            pltpu.SemaphoreType.DMA((COPIES,)),
            pltpu.SemaphoreType.DMA((4, 4, 2)),
        ],
        compiler_params=pltpu.CompilerParams(
            collective_id=number, has_side_effects=True, vmem_limit_bytes=48 * 1024 * 1024
        ),
        cost_estimate=pl.CostEstimate(
            flops=2 * cap * 1024 * 1024, bytes_accessed=3 << 20, transcendentals=0
        ),
        name=f"wgrad{cap}",
    )


def shards(attn_out, out_grad, valid_counts):
    hbm = pl.BlockSpec(memory_space=pltpu.HBM)
    vmem = pl.BlockSpec(memory_space=pltpu.VMEM)
    grains = [value.reshape(TOK // GRAIN, GRAIN, BLK) for value in (attn_out, out_grad)]
    turned, packed, which = pl.pallas_call(
        compact,
        out_shape=(
            jax.ShapeDtypeStruct((BLK, TOK), attn_out.dtype),
            jax.ShapeDtypeStruct((TOK, BLK), out_grad.dtype),
            jax.ShapeDtypeStruct((1,), jnp.int32),
        ),
        in_specs=[hbm, hbm, hbm],
        out_specs=(vmem, vmem, pl.BlockSpec(memory_space=pltpu.SMEM)),
        scratch_shapes=[
            pltpu.SMEM((TOK // SEQ,), jnp.int32),
            pltpu.VMEM((TOK // GRAIN, GRAIN, BLK), jnp.bfloat16),
            pltpu.VMEM((TOK // GRAIN, GRAIN, BLK), jnp.bfloat16),
            pltpu.VMEM((8, BLK), jnp.int32),
            pltpu.VMEM((3, 8, BLK), jnp.int32),
            pltpu.SemaphoreType.DMA,
            pltpu.SemaphoreType.DMA((2, TOK // SEQ)),
            pltpu.SemaphoreType.DMA((3,)),
            pltpu.SemaphoreType.DMA((3,)),
        ],
        compiler_params=pltpu.CompilerParams(
            collective_id=0, has_side_effects=True, vmem_limit_bytes=16 * 1024 * 1024
        ),
        name="compact",
    )(*(pltpu.with_memory_space_constraint(value, pltpu.HBM) for value in (valid_counts, *grains)))
    branches = [main(cap, 1 + i) for i, cap in enumerate(CAPS)]
    return lax.switch(which[0], branches, turned, packed)


def solution(mesh):
    return jax.shard_map(
        shards,
        mesh=mesh,
        in_specs=(P("gx", ("gy", "gz")), P("gx", ("gz", "gy")), P("gx")),
        out_specs=P(("gy", "gx"), "gz"),
        check_vma=False,
    )
```

```python
import functools

import jax
import jax.numpy as jnp
from jax import lax
from jax.experimental import pallas as pl
from jax.experimental.pallas import tpu as pltpu
from jax.sharding import PartitionSpec as P

MESH = pl.DeviceIdType.MESH
TOK = 4096
SEQ = 1024
BLK = 128
GRAIN = 16
CAPS = (2176, 2304, 2432, 2560, 2688, 2816, 2944, 3072, 3200, 3328, 3456, 3584, 3712, 4096)
UNROLL = 4
COPIES = 32


def compact(vc_hbm, a_hbm, b_hbm, at_out, b_out, which, vc, raw_a, raw_b, mine, theirs, csem, lsem, ss, rs):
    zl = lax.axis_index("gx")
    gy = lax.axis_index("gy")
    gz = lax.axis_index("gz")
    rows_here = TOK // SEQ
    barrier = pltpu.get_barrier_semaphore()
    peers = [((zl + d) % 4, gy, gz) for d in range(1, 4)]
    for dev in peers:
        pl.semaphore_signal(barrier, inc=1, device_id=dev, device_id_type=MESH)
    counts = pltpu.make_async_copy(vc_hbm, vc, csem)
    counts.start()
    loads = []
    for r in range(rows_here):
        part = pl.ds(r * (SEQ // GRAIN), SEQ // GRAIN)
        loads.append(pltpu.make_async_copy(a_hbm.at[part], raw_a.at[part], lsem.at[0, r]))
        loads.append(pltpu.make_async_copy(b_hbm.at[part], raw_b.at[part], lsem.at[1, r]))
    for load in loads:
        load.start()
    counts.wait()
    valid = [vc[r] for r in range(rows_here)]
    first = [0]
    for r in range(rows_here):
        first.append(first[-1] + (valid[r] + GRAIN - 1) // GRAIN)
    mine[...] = jnp.full(mine.shape, first[-1] * GRAIN, jnp.int32)
    pl.semaphore_wait(barrier, len(peers))
    copies = [
        pltpu.make_async_remote_copy(
            src_ref=mine, dst_ref=theirs.at[d], send_sem=ss.at[d], recv_sem=rs.at[d],
            device_id=peers[d], device_id_type=MESH,
        )
        for d in range(3)
    ]
    for copy in copies:
        copy.start()
    for load in loads:
        load.wait()

    shift = [r * (SEQ // GRAIN) - first[r] for r in range(rows_here)]
    limit = [valid[r] + first[r] * GRAIN for r in range(rows_here)]
    token = lax.broadcasted_iota(jnp.int32, (GRAIN, BLK), 0)

    def tile(k):
        pieces = []
        for i in range(BLK // GRAIN):
            n = k * (BLK // GRAIN) + i
            move, end = shift[0], limit[0]
            for r in range(1, rows_here):
                past = n >= first[r]
                move = jnp.where(past, shift[r], move)
                end = jnp.where(past, limit[r], end)
            source = jnp.minimum(n + move, TOK // GRAIN - 1)
            piece = raw_a[source]
            pieces.append(jnp.where(token < end - n * GRAIN, piece, jnp.zeros((), piece.dtype)))
            b_out[pl.ds(pl.multiple_of(n * GRAIN, GRAIN), GRAIN), :] = raw_b[source]
        span = pl.ds(pl.multiple_of(k * BLK, BLK), BLK)
        at_out[:, span] = jnp.concatenate(pieces, axis=0).T

    def tiles(k, carry):
        for i in range(UNROLL):
            tile(k * UNROLL + i)
        return carry

    lax.fori_loop(0, TOK // BLK // UNROLL, tiles, 0)
    for copy in copies:
        copy.wait_recv()
    most = first[-1] * GRAIN
    for d in range(3):
        most = jnp.maximum(most, theirs[d, 0, 0])
    index = 0
    for cap in CAPS[:-1]:
        index = index + jnp.where(most > cap, 1, 0)
    which[0] = index
    for copy in copies:
        copy.wait_send()


def kernel(cap, a_hbm, b_hbm, result, out, at, bb, sbuf, rbuf, ssc, rsc, acc, lsem, osem, sent, rs, prs):
    CHK, HALF = cap // 4, cap // 2
    zl = lax.axis_index("gx")
    gy = lax.axis_index("gy")
    gz = lax.axis_index("gz")
    x, zh = gy // 2, gy % 2
    y, c = gz // 2, gz % 2
    xr, xl, xo = (x + 1) % 4, (x + 3) % 4, (x + 2) % 4
    yr, yl, yo = (y + 1) % 4, (y + 3) % 4, (y + 2) % 4

    right, left = (zl, xr * 2 + zh, gz), (zl, xl * 2 + zh, gz)
    far = (zl, x * 2 + (1 - zh), gz)
    up, down = (zl, gy, yr * 2 + c), (zl, gy, yl * 2 + c)
    sibling = (zl, gy, y * 2 + (1 - c))
    owners = [((zl + d) % 4, gy, gz) for d in range(1, 4)]

    barrier = pltpu.get_barrier_semaphore()
    partners = [far, right, left, up, down, sibling] + owners
    for dev in partners:
        pl.semaphore_signal(barrier, inc=1, device_id=dev, device_id_type=MESH)

    def rows(block, h=None):
        if h is None:
            return pl.ds(pl.multiple_of(block * BLK, BLK), BLK)
        return pl.ds(pl.multiple_of(block * BLK + h * (BLK // 2), BLK // 2), BLK // 2)

    load_a = pltpu.make_async_copy(a_hbm.at[:, pl.ds(0, cap)], at.at[rows(gz)], lsem.at[0])
    load_b = pltpu.make_async_copy(b_hbm.at[pl.ds(0, cap)], bb.at[gy], lsem.at[1])
    load_a.start()
    load_b.start()
    pl.semaphore_wait(barrier, len(partners))

    made = []

    def remote(src, dst, dev, kind=0):
        k = len(made)
        copy = pltpu.make_async_remote_copy(
            src_ref=src,
            dst_ref=dst,
            send_sem=sent.at[kind],
            recv_sem=rs.at[k],
            device_id=dev,
            device_id_type=MESH,
        )
        made.append(copy)
        return copy

    def tokens(q, size):
        return pl.ds(q * size, size)

    far_q = {q: remote(b_hbm.at[tokens(q, CHK)], bb.at[gy, tokens(q, CHK)], far) for q in range(4)}
    own_r = {h: remote(b_hbm.at[tokens(h, HALF)], bb.at[gy, tokens(h, HALF)], right) for h in range(2)}
    own_l = {h: remote(b_hbm.at[tokens(h, HALF)], bb.at[gy, tokens(h, HALF)], left) for h in range(2)}

    def relay(slot, q, size, dev):
        return remote(bb.at[slot, tokens(q, size)], bb.at[slot, tokens(q, size)], dev)

    hop_r = relay(xl * 2 + zh, 0, HALF, right)
    hop_l = relay(xr * 2 + zh, 1, HALF, left)
    oz = 1 - zh
    far_r = {q: relay(x * 2 + oz, q, CHK, right) for q in range(4)}
    far_l = {q: relay(x * 2 + oz, q, CHK, left) for q in range(4)}
    fhop_r = {q: relay(xl * 2 + oz, q, CHK, right) for q in (0, 1)}
    fhop_l = {q: relay(xr * 2 + oz, q, CHK, left) for q in (2, 3)}

    def pass_on(block, h, dev):
        return remote(at.at[rows(block, h)], at.at[rows(block, h)], dev, 1)

    def own(h, dev):
        part = pl.ds(h * (BLK // 2), BLK // 2)
        return remote(a_hbm.at[part, pl.ds(0, cap)], at.at[rows(gz, h)], dev, 1)

    a_up = {h: own(h, up) for h in range(2)}
    a_down = {h: own(h, down) for h in range(2)}
    ahop_up = pass_on(yl * 2 + c, 0, up)
    ahop_down = pass_on(yr * 2 + c, 1, down)
    sib = {d: pass_on(((y + d) % 4) * 2 + c, None, sibling) for d in range(1, 4)}
    sib[0] = remote(a_hbm.at[:, pl.ds(0, cap)], at.at[rows(gz)], sibling, 1)

    for q in (0, 2, 1, 3):
        far_q[q].start()
    own_r[0].start()
    own_l[1].start()
    own_r[1].start()
    own_l[0].start()

    a_up[0].start()
    a_down[1].start()
    a_up[1].start()
    a_down[0].start()
    sib[0].start()

    own_r[0].wait_recv()
    hop_r.start()
    own_l[1].wait_recv()
    hop_l.start()
    a_up[0].wait_recv()
    ahop_up.start()
    a_down[1].wait_recv()
    ahop_down.start()
    far_q[0].wait_recv()
    far_r[0].start()
    far_l[0].start()
    a_up[1].wait_recv()
    sib[3].start()
    a_down[0].wait_recv()
    sib[1].start()
    far_q[2].wait_recv()
    far_r[2].start()
    far_l[2].start()
    ahop_up.wait_recv()
    ahop_down.wait_recv()
    sib[2].start()
    far_q[1].wait_recv()
    far_r[1].start()
    far_l[1].start()
    for d in range(4):
        sib[d].wait_recv()

    side = zl // 2
    mid = (zl + side) % 2
    end_at, mid_at, far_mid, far_end = 3 * side, 1 + side, 2 - side, 3 - 3 * side
    goal = [
        mid * far_mid + (1 - mid) * far_end,
        mid * end_at + (1 - mid) * far_mid,
        mid * far_end + (1 - mid) * mid_at,
    ]
    goes_to = [
        mid * far_mid + (1 - mid) * mid_at,
        mid * end_at + (1 - mid) * far_mid,
        mid * far_end + (1 - mid) * mid_at,
    ]
    lands = [3 * (1 - mid), 1 - mid, 2 - mid]

    blocks = [gy, xr * 2 + zh, xl * 2 + zh, xo * 2 + zh, x * 2 + oz, xr * 2 + oz, xl * 2 + oz, xo * 2 + oz]

    def pick(choices, k):
        if isinstance(k, int):
            return choices[k]
        value = choices[-1]
        for i in range(len(choices) - 1):
            value = jnp.where(k == i, choices[i], value)
        return value

    def part_copies(k, u, slot):
        span = pl.ds(2 * u, 2)
        dev = (pick(goes_to, k), gy, gz)
        return [
            pltpu.make_async_remote_copy(
                src_ref=src.at[k, span],
                dst_ref=dst.at[slot, span],
                send_sem=sent.at[2 + w],
                recv_sem=prs.at[slot, u, w],
                device_id=dev,
                device_id_type=MESH,
            )
            for w, (src, dst) in enumerate(((sbuf, rbuf), (ssc, rsc)))
        ]

    def columns(u, i):
        return pl.ds(pl.multiple_of(pick(blocks[i::2], u) * BLK, BLK), BLK)

    def product(chunk, u):
        lhs = at[pl.ds(pl.multiple_of(chunk * 2 * BLK, 2 * BLK), 2 * BLK), :]
        rhs = jnp.concatenate([bb[pick(blocks[i::2], u)] for i in range(2)], axis=1)
        part = jnp.dot(lhs, rhs, preferred_element_type=jnp.float32)
        return [part[:, :BLK], part[:, BLK:]]

    def send(k, u, parts):
        for i in range(2):
            top = jnp.maximum(jnp.max(jnp.abs(parts[i]), axis=0, keepdims=True), 2e-34)
            sbuf[k, 2 * u + i] = jnp.round(parts[i] * (32767.0 / top)).astype(jnp.int32).astype(jnp.int16)
            ssc[k, 2 * u + i] = top * (1.0 / 32767.0)
        for copy in part_copies(k, u, pick(lands, k)):
            copy.start()

    def arrived(slot, u):
        for copy in part_copies(0, u, slot):
            copy.wait_recv()
        return [
            rbuf[slot, 2 * u + i].astype(jnp.int32).astype(jnp.float32) * rsc[slot, 2 * u + i]
            for i in range(2)
        ]

    def unit(u):
        def step(k, carry):
            parts = product(pick(goal + [zl], k), u)
            held = jnp.logical_and(k == 2, mid == 1)

            @pl.when(jnp.logical_and(k < 3, jnp.logical_not(held)))
            def _():
                send(k, u, parts)

            @pl.when(held)
            def _():
                for i in range(2):
                    acc[2 * u + i] = parts[i]

            @pl.when(k == 3)
            def _():
                for i in range(2):
                    out[:, columns(u, i)] = parts[i]

            return carry

        lax.fori_loop(0, 4, step, 0)

    def finish(u):
        parts = arrived(3, u)
        send(2, u, [acc[2 * u + i] + parts[i] for i in range(2)])

    def stores(u):
        return [
            pltpu.make_async_copy(out.at[:, columns(u, i)], result.at[:, columns(u, i)], osem)
            for i in range(2)
        ]

    def gather(u, carry):
        def add(slot):
            parts = arrived(slot, u)
            for i in range(2):
                out[:, columns(u, i)] += parts[i]

        add(0)

        @pl.when(mid == 1)
        def _():
            add(2)

        add(1)
        for copy in stores(u):
            copy.start()
        return carry

    def stage(u, carry):
        @pl.when(u == 0)
        def _():
            load_a.wait()
            load_b.wait()
            own_l[0].wait_recv()

        @pl.when(u == 1)
        def _():
            far_q[3].wait_recv()
            far_r[3].start()
            far_l[3].start()
            far_r[0].wait_recv()
            fhop_r[0].start()
            far_l[2].wait_recv()
            fhop_l[2].start()
            own_r[1].wait_recv()
            hop_r.wait_recv()
            hop_l.wait_recv()

        @pl.when(u == 2)
        def _():
            far_r[1].wait_recv()
            fhop_r[1].start()
            far_l[3].wait_recv()
            fhop_l[3].start()
            far_l[0].wait_recv()
            far_l[1].wait_recv()

        @pl.when(u == 3)
        def _():
            far_r[2].wait_recv()
            far_r[3].wait_recv()
            fhop_r[0].wait_recv()
            fhop_r[1].wait_recv()
            fhop_l[2].wait_recv()
            fhop_l[3].wait_recv()

        unit(u)

        @pl.when(jnp.logical_and(u > 0, mid == 1))
        def _():
            finish(u - 1)

        return carry

    lax.fori_loop(0, 4, stage, 0)

    @pl.when(mid == 1)
    def _():
        finish(3)

    lax.fori_loop(0, 4, gather, 0)
    pltpu.make_async_copy(out, result, osem).wait()
    pltpu.make_async_copy(bb.at[pl.ds(0, 7)], bb.at[pl.ds(0, 7)], sent.at[0]).wait()
    pltpu.make_async_copy(at.at[pl.ds(0, 7 * BLK)], at.at[pl.ds(0, 7 * BLK)], sent.at[1]).wait()
    pltpu.make_async_copy(sbuf, sbuf, sent.at[2]).wait()
    pltpu.make_async_copy(ssc, ssc, sent.at[3]).wait()


def main(cap, number):
    any_space = pl.BlockSpec(memory_space=pl.ANY)
    return pl.pallas_call(
        functools.partial(kernel, cap),
        out_shape=jax.ShapeDtypeStruct((2 * BLK, 8 * BLK), jnp.float32),
        in_specs=[any_space] * 2,
        out_specs=any_space,
        scratch_shapes=[
            pltpu.VMEM((2 * BLK, 8 * BLK), jnp.float32),
            pltpu.VMEM((8 * BLK, cap), jnp.bfloat16),
            pltpu.VMEM((8, cap, BLK), jnp.bfloat16),
            pltpu.VMEM((3, 8, 2 * BLK, BLK), jnp.int16),
            pltpu.VMEM((4, 8, 2 * BLK, BLK), jnp.int16),
            pltpu.VMEM((3, 8, 1, BLK), jnp.float32),
            pltpu.VMEM((4, 8, 1, BLK), jnp.float32),
            pltpu.VMEM((8, 2 * BLK, BLK), jnp.float32),
            pltpu.SemaphoreType.DMA((2,)),
            pltpu.SemaphoreType.DMA,
            pltpu.SemaphoreType.DMA((4,)),
            pltpu.SemaphoreType.DMA((COPIES,)),
            pltpu.SemaphoreType.DMA((4, 4, 2)),
        ],
        compiler_params=pltpu.CompilerParams(
            collective_id=number, has_side_effects=True, vmem_limit_bytes=48 * 1024 * 1024
        ),
        cost_estimate=pl.CostEstimate(
            flops=2 * cap * 1024 * 1024, bytes_accessed=3 << 20, transcendentals=0
        ),
        name=f"wgrad{cap}",
    )


def shards(attn_out, out_grad, valid_counts):
    hbm = pl.BlockSpec(memory_space=pltpu.HBM)
    vmem = pl.BlockSpec(memory_space=pltpu.VMEM)
    grains = [value.reshape(TOK // GRAIN, GRAIN, BLK) for value in (attn_out, out_grad)]
    turned, packed, which = pl.pallas_call(
        compact,
        out_shape=(
            jax.ShapeDtypeStruct((BLK, TOK), attn_out.dtype),
            jax.ShapeDtypeStruct((TOK, BLK), out_grad.dtype),
            jax.ShapeDtypeStruct((1,), jnp.int32),
        ),
        in_specs=[hbm, hbm, hbm],
        out_specs=(vmem, vmem, pl.BlockSpec(memory_space=pltpu.SMEM)),
        scratch_shapes=[
            pltpu.SMEM((TOK // SEQ,), jnp.int32),
            pltpu.VMEM((TOK // GRAIN, GRAIN, BLK), jnp.bfloat16),
            pltpu.VMEM((TOK // GRAIN, GRAIN, BLK), jnp.bfloat16),
            pltpu.VMEM((8, BLK), jnp.int32),
            pltpu.VMEM((3, 8, BLK), jnp.int32),
            pltpu.SemaphoreType.DMA,
            pltpu.SemaphoreType.DMA((2, TOK // SEQ)),
            pltpu.SemaphoreType.DMA((3,)),
            pltpu.SemaphoreType.DMA((3,)),
        ],
        compiler_params=pltpu.CompilerParams(
            collective_id=0, has_side_effects=True, vmem_limit_bytes=16 * 1024 * 1024
        ),
        name="compact",
    )(*(pltpu.with_memory_space_constraint(value, pltpu.HBM) for value in (valid_counts, *grains)))
    branches = [main(cap, 1 + i) for i, cap in enumerate(CAPS)]
    return lax.switch(which[0], branches, turned, packed)


def solution(mesh):
    return jax.shard_map(
        shards,
        mesh=mesh,
        in_specs=(P("gx", ("gy", "gz")), P("gx", ("gz", "gy")), P("gx")),
        out_specs=P(("gy", "gx"), "gz"),
        check_vma=False,
    )
```

```python
import functools

import jax
import jax.numpy as jnp
from jax import lax
from jax.experimental import pallas as pl
from jax.experimental.pallas import tpu as pltpu
from jax.sharding import PartitionSpec as P

MESH = pl.DeviceIdType.MESH
TOK = 4096
SEQ = 1024
BLK = 128
GRAIN = 16
PLANS = (
    (2304, 2304, 2560, 2560), (2560, 2560, 2432, 2432), (2944, 2176, 2944, 2176), (2560, 2688, 2688, 2688),
    (2816, 2816, 2816, 2432), (2304, 2304, 3072, 3072), (2432, 3072, 2432, 3072), (2944, 2560, 2944, 2944),
    (3200, 3200, 2560, 2560), (2688, 2688, 3328, 3328), (3072, 3072, 3072, 3072), (2688, 3584, 2688, 3584),
    (3712, 2688, 3712, 2688), (3456, 3456, 3456, 3200), (3840, 3840, 2944, 3840), (4096, 4096, 4096, 4096),
)
UNROLL = 4
COPIES = 37


def compact(vc_hbm, a_hbm, b_hbm, at_out, b_out, which, vc, raw_a, raw_b, mine, theirs, csem, lsem, ss, rs):
    zl = lax.axis_index("gx")
    gy = lax.axis_index("gy")
    gz = lax.axis_index("gz")
    rows_here = TOK // SEQ
    barrier = pltpu.get_barrier_semaphore()
    peers = [((zl + d) % 4, gy, gz) for d in range(1, 4)]
    for dev in peers:
        pl.semaphore_signal(barrier, inc=1, device_id=dev, device_id_type=MESH)
    counts = pltpu.make_async_copy(vc_hbm, vc, csem)
    counts.start()
    loads = []
    for r in range(rows_here):
        part = pl.ds(r * (SEQ // GRAIN), SEQ // GRAIN)
        loads.append(pltpu.make_async_copy(a_hbm.at[part], raw_a.at[part], lsem.at[0, r]))
        loads.append(pltpu.make_async_copy(b_hbm.at[part], raw_b.at[part], lsem.at[1, r]))
    for load in loads:
        load.start()
    counts.wait()
    valid = [vc[r] for r in range(rows_here)]
    first = [0]
    for r in range(rows_here):
        first.append(first[-1] + (valid[r] + GRAIN - 1) // GRAIN)
    mine[...] = jnp.full(mine.shape, first[-1] * GRAIN, jnp.int32)
    pl.semaphore_wait(barrier, len(peers))
    copies = [
        pltpu.make_async_remote_copy(
            src_ref=mine, dst_ref=theirs.at[d], send_sem=ss.at[d], recv_sem=rs.at[d],
            device_id=peers[d], device_id_type=MESH,
        )
        for d in range(3)
    ]
    for copy in copies:
        copy.start()
    for load in loads:
        load.wait()

    shift = [r * (SEQ // GRAIN) - first[r] for r in range(rows_here)]
    limit = [valid[r] + first[r] * GRAIN for r in range(rows_here)]
    token = lax.broadcasted_iota(jnp.int32, (GRAIN, BLK), 0)

    def tile(k):
        pieces = []
        for i in range(BLK // GRAIN):
            n = k * (BLK // GRAIN) + i
            move, end = shift[0], limit[0]
            for r in range(1, rows_here):
                past = n >= first[r]
                move = jnp.where(past, shift[r], move)
                end = jnp.where(past, limit[r], end)
            source = jnp.minimum(n + move, TOK // GRAIN - 1)
            piece = raw_a[source]
            pieces.append(jnp.where(token < end - n * GRAIN, piece, jnp.zeros((), piece.dtype)))
            b_out[pl.ds(pl.multiple_of(n * GRAIN, GRAIN), GRAIN), :] = raw_b[source]
        span = pl.ds(pl.multiple_of(k * BLK, BLK), BLK)
        at_out[:, span] = jnp.concatenate(pieces, axis=0).T

    def tiles(k, carry):
        for i in range(UNROLL):
            tile(k * UNROLL + i)
        return carry

    lax.fori_loop(0, TOK // BLK // UNROLL, tiles, 0)
    for copy in copies:
        copy.wait_recv()
    totals = [first[-1] * GRAIN] + [theirs[d, 0, 0] for d in range(3)]
    group = []
    for g in range(4):
        back, value = (zl + 4 - g) % 4, totals[3]
        for d in range(3):
            value = jnp.where(back == d, totals[d], value)
        group.append(value)
    index = len(PLANS) - 1
    for n in reversed(range(len(PLANS) - 1)):
        short = sum(jnp.where(group[g] > PLANS[n][g], 1, 0) for g in range(4))
        index = jnp.where(short == 0, n, index)
    which[0] = index
    for copy in copies:
        copy.wait_send()


def kernel(plan, a_hbm, b_hbm, result, out, at, bb, sbuf, rbuf, ssc, rsc, acc, lsem, osem, sent, rs, prs):
    cap, low = max(plan), min(plan)
    CHK, HALF = low // 4, cap // 2
    zl = lax.axis_index("gx")
    gy = lax.axis_index("gy")
    gz = lax.axis_index("gz")
    x, zh = gy // 2, gy % 2
    y, c = gz // 2, gz % 2
    xr, xl, xo = (x + 1) % 4, (x + 3) % 4, (x + 2) % 4
    yr, yl, yo = (y + 1) % 4, (y + 3) % 4, (y + 2) % 4

    right, left = (zl, xr * 2 + zh, gz), (zl, xl * 2 + zh, gz)
    far = (zl, x * 2 + (1 - zh), gz)
    up, down = (zl, gy, yr * 2 + c), (zl, gy, yl * 2 + c)
    sibling = (zl, gy, y * 2 + (1 - c))
    owners = [((zl + d) % 4, gy, gz) for d in range(1, 4)]

    barrier = pltpu.get_barrier_semaphore()
    partners = [far, right, left, up, down, sibling] + owners
    for dev in partners:
        pl.semaphore_signal(barrier, inc=1, device_id=dev, device_id_type=MESH)

    def rows(block, h=None):
        if h is None:
            return pl.ds(pl.multiple_of(block * BLK, BLK), BLK)
        return pl.ds(pl.multiple_of(block * BLK + h * (BLK // 2), BLK // 2), BLK // 2)

    load_a = pltpu.make_async_copy(a_hbm.at[:, pl.ds(0, cap)], at.at[rows(gz)], lsem.at[0])
    load_b = pltpu.make_async_copy(b_hbm.at[pl.ds(0, cap)], bb.at[gy], lsem.at[1])
    load_a.start()
    load_b.start()
    pl.semaphore_wait(barrier, len(partners))

    made = []

    def remote(src, dst, dev, kind=4):
        k = len(made)
        copy = pltpu.make_async_remote_copy(
            src_ref=src,
            dst_ref=dst,
            send_sem=sent.at[kind],
            recv_sem=rs.at[k],
            device_id=dev,
            device_id_type=MESH,
        )
        made.append(copy)
        return copy

    def tokens(q, size):
        return pl.ds(q * size, size)

    far_q = {q: remote(b_hbm.at[tokens(q, CHK)], bb.at[gy, tokens(q, CHK)], far) for q in range(4)}
    own_r = {h: remote(b_hbm.at[tokens(h, HALF)], bb.at[gy, tokens(h, HALF)], right, 0) for h in range(2)}
    own_l = {h: remote(b_hbm.at[tokens(h, HALF)], bb.at[gy, tokens(h, HALF)], left, 0) for h in range(2)}

    def relay(slot, q, size, dev, kind=4):
        return remote(bb.at[slot, tokens(q, size)], bb.at[slot, tokens(q, size)], dev, kind)

    hop_r = relay(xl * 2 + zh, 0, HALF, right, 0)
    hop_l = relay(xr * 2 + zh, 1, HALF, left, 0)
    oz = 1 - zh
    far_r = {q: relay(x * 2 + oz, q, CHK, right) for q in range(4)}
    far_l = {q: relay(x * 2 + oz, q, CHK, left) for q in range(4)}
    fhop_r = {q: relay(xl * 2 + oz, q, CHK, right) for q in (0, 1)}
    fhop_l = {q: relay(xr * 2 + oz, q, CHK, left) for q in (2, 3)}

    tail = pl.ds(low, cap - low)
    large = functools.reduce(jnp.logical_or, [zl == g for g in range(4) if plan[g] == cap])

    def larger(do):
        if low < cap:
            pl.when(large)(do)

    def more(slot, begin, size, dev):
        part = pl.ds(begin, size)
        return remote(bb.at[slot, part], bb.at[slot, part], dev, 5)

    if low < cap:
        rest = (cap - low) // 2
        tail_far = remote(b_hbm.at[tail], bb.at[gy, tail], far, 5)
        tail_r = more(x * 2 + oz, low, cap - low, right)
        tail_l = more(x * 2 + oz, low, cap - low, left)
        tail_hop_r = more(xl * 2 + oz, low, rest, right)
        tail_hop_l = more(xr * 2 + oz, low + rest, rest, left)

    def pass_on(block, h, dev):
        return remote(at.at[rows(block, h)], at.at[rows(block, h)], dev, 1)

    def own(h, dev):
        part = pl.ds(h * (BLK // 2), BLK // 2)
        return remote(a_hbm.at[part, pl.ds(0, cap)], at.at[rows(gz, h)], dev, 1)

    a_up = {h: own(h, up) for h in range(2)}
    a_down = {h: own(h, down) for h in range(2)}
    ahop_up = pass_on(yl * 2 + c, 0, up)
    ahop_down = pass_on(yr * 2 + c, 1, down)
    sib = {d: pass_on(((y + d) % 4) * 2 + c, None, sibling) for d in range(1, 4)}
    sib[0] = remote(a_hbm.at[:, pl.ds(0, cap)], at.at[rows(gz)], sibling, 1)

    for q in (0, 2, 1, 3):
        far_q[q].start()

    @larger
    def _():
        tail_far.start()

    own_r[0].start()
    own_l[1].start()
    own_r[1].start()
    own_l[0].start()

    a_up[0].start()
    a_down[1].start()
    a_up[1].start()
    a_down[0].start()
    sib[0].start()

    if low < cap:

        @pl.when(jnp.logical_not(large))
        def _():
            def blank(n, carry):
                part = pl.ds(pl.multiple_of(low + n * BLK, BLK), BLK)
                for v in range(4):
                    bb[v * 2 + oz, part, :] = jnp.zeros((BLK, BLK), bb.dtype)
                return carry

            lax.fori_loop(0, (cap - low) // BLK, blank, 0)

    own_r[0].wait_recv()
    hop_r.start()
    own_l[1].wait_recv()
    hop_l.start()
    a_up[0].wait_recv()
    ahop_up.start()
    a_down[1].wait_recv()
    ahop_down.start()
    far_q[0].wait_recv()
    far_r[0].start()
    far_l[0].start()
    a_up[1].wait_recv()
    sib[3].start()
    a_down[0].wait_recv()
    sib[1].start()
    far_q[2].wait_recv()
    far_r[2].start()
    far_l[2].start()
    ahop_up.wait_recv()
    ahop_down.wait_recv()
    sib[2].start()
    far_q[1].wait_recv()
    far_r[1].start()
    far_l[1].start()
    for d in range(4):
        sib[d].wait_recv()

    side = zl // 2
    mid = (zl + side) % 2
    end_at, mid_at, far_mid, far_end = 3 * side, 1 + side, 2 - side, 3 - 3 * side
    goal = [
        mid * far_mid + (1 - mid) * far_end,
        mid * end_at + (1 - mid) * far_mid,
        mid * far_end + (1 - mid) * mid_at,
    ]
    goes_to = [
        mid * far_mid + (1 - mid) * mid_at,
        mid * end_at + (1 - mid) * far_mid,
        mid * far_end + (1 - mid) * mid_at,
    ]
    lands = [3 * (1 - mid), 1 - mid, 2 - mid]

    blocks = [gy, xr * 2 + zh, xl * 2 + zh, xo * 2 + zh, x * 2 + oz, xr * 2 + oz, xl * 2 + oz, xo * 2 + oz]

    def pick(choices, k):
        if isinstance(k, int):
            return choices[k]
        value = choices[-1]
        for i in range(len(choices) - 1):
            value = jnp.where(k == i, choices[i], value)
        return value

    def part_copies(k, u, slot):
        span = pl.ds(2 * u, 2)
        dev = (pick(goes_to, k), gy, gz)
        return [
            pltpu.make_async_remote_copy(
                src_ref=src.at[k, span],
                dst_ref=dst.at[slot, span],
                send_sem=sent.at[2 + w],
                recv_sem=prs.at[slot, u, w],
                device_id=dev,
                device_id_type=MESH,
            )
            for w, (src, dst) in enumerate(((sbuf, rbuf), (ssc, rsc)))
        ]

    def columns(u, i):
        return pl.ds(pl.multiple_of(pick(blocks[i::2], u) * BLK, BLK), BLK)

    def product(chunk, u):
        lhs = at[pl.ds(pl.multiple_of(chunk * 2 * BLK, 2 * BLK), 2 * BLK), :]
        rhs = jnp.concatenate([bb[pick(blocks[i::2], u)] for i in range(2)], axis=1)
        part = jnp.dot(lhs, rhs, preferred_element_type=jnp.float32)
        return [part[:, :BLK], part[:, BLK:]]

    def send(k, u, parts):
        for i in range(2):
            top = jnp.maximum(jnp.max(jnp.abs(parts[i]), axis=0, keepdims=True), 2e-34)
            sbuf[k, 2 * u + i] = jnp.round(parts[i] * (32767.0 / top)).astype(jnp.int32).astype(jnp.int16)
            ssc[k, 2 * u + i] = top * (1.0 / 32767.0)
        for copy in part_copies(k, u, pick(lands, k)):
            copy.start()

    def arrived(slot, u):
        for copy in part_copies(0, u, slot):
            copy.wait_recv()
        return [
            rbuf[slot, 2 * u + i].astype(jnp.int32).astype(jnp.float32) * rsc[slot, 2 * u + i]
            for i in range(2)
        ]

    def unit(u):
        def step(k, carry):
            parts = product(pick(goal + [zl], k), u)
            held = jnp.logical_and(k == 2, mid == 1)

            @pl.when(jnp.logical_and(k < 3, jnp.logical_not(held)))
            def _():
                send(k, u, parts)

            @pl.when(held)
            def _():
                for i in range(2):
                    acc[2 * u + i] = parts[i]

            @pl.when(k == 3)
            def _():
                for i in range(2):
                    out[:, columns(u, i)] = parts[i]

            return carry

        lax.fori_loop(0, 4, step, 0)

    def finish(u):
        parts = arrived(3, u)
        send(2, u, [acc[2 * u + i] + parts[i] for i in range(2)])

    def stores(u):
        return [
            pltpu.make_async_copy(out.at[:, columns(u, i)], result.at[:, columns(u, i)], osem)
            for i in range(2)
        ]

    def gather(u, carry):
        def add(slot):
            parts = arrived(slot, u)
            for i in range(2):
                out[:, columns(u, i)] += parts[i]

        add(0)

        @pl.when(mid == 1)
        def _():
            add(2)

        add(1)
        for copy in stores(u):
            copy.start()
        return carry

    def stage(u, carry):
        @pl.when(u == 0)
        def _():
            load_a.wait()
            load_b.wait()
            own_l[0].wait_recv()

        @pl.when(u == 1)
        def _():
            far_q[3].wait_recv()
            far_r[3].start()
            far_l[3].start()

            @larger
            def _():
                tail_far.wait_recv()
                tail_r.start()
                tail_l.start()

            far_r[0].wait_recv()
            fhop_r[0].start()
            far_l[2].wait_recv()
            fhop_l[2].start()
            own_r[1].wait_recv()
            hop_r.wait_recv()
            hop_l.wait_recv()

        @pl.when(u == 2)
        def _():
            far_r[1].wait_recv()
            fhop_r[1].start()
            far_l[3].wait_recv()
            fhop_l[3].start()
            far_l[0].wait_recv()
            far_l[1].wait_recv()

            @larger
            def _():
                tail_r.wait_recv()
                tail_hop_r.start()
                tail_l.wait_recv()
                tail_hop_l.start()


        @pl.when(u == 3)
        def _():
            far_r[2].wait_recv()
            far_r[3].wait_recv()
            fhop_r[0].wait_recv()
            fhop_r[1].wait_recv()
            fhop_l[2].wait_recv()
            fhop_l[3].wait_recv()

            @larger
            def _():
                tail_hop_r.wait_recv()
                tail_hop_l.wait_recv()

        unit(u)

        @pl.when(jnp.logical_and(u > 0, mid == 1))
        def _():
            finish(u - 1)

        return carry

    lax.fori_loop(0, 4, stage, 0)

    @pl.when(mid == 1)
    def _():
        finish(3)

    lax.fori_loop(0, 4, gather, 0)
    pltpu.make_async_copy(out, result, osem).wait()
    exchanged = bb.at[pl.ds(0, 4), pl.ds(0, low)]
    pltpu.make_async_copy(bb.at[pl.ds(0, 3)], bb.at[pl.ds(0, 3)], sent.at[0]).wait()
    pltpu.make_async_copy(exchanged, exchanged, sent.at[4]).wait()

    @larger
    def _():
        beyond = bb.at[pl.ds(0, 4), tail]
        pltpu.make_async_copy(beyond, beyond, sent.at[5]).wait()

    pltpu.make_async_copy(at.at[pl.ds(0, 7 * BLK)], at.at[pl.ds(0, 7 * BLK)], sent.at[1]).wait()
    pltpu.make_async_copy(sbuf, sbuf, sent.at[2]).wait()
    pltpu.make_async_copy(ssc, ssc, sent.at[3]).wait()


def main(plan, number):
    cap = max(plan)
    any_space = pl.BlockSpec(memory_space=pl.ANY)
    return pl.pallas_call(
        functools.partial(kernel, plan),
        out_shape=jax.ShapeDtypeStruct((2 * BLK, 8 * BLK), jnp.float32),
        in_specs=[any_space] * 2,
        out_specs=any_space,
        scratch_shapes=[
            pltpu.VMEM((2 * BLK, 8 * BLK), jnp.float32),
            pltpu.VMEM((8 * BLK, cap), jnp.bfloat16),
            pltpu.VMEM((8, cap, BLK), jnp.bfloat16),
            pltpu.VMEM((3, 8, 2 * BLK, BLK), jnp.int16),
            pltpu.VMEM((4, 8, 2 * BLK, BLK), jnp.int16),
            pltpu.VMEM((3, 8, 1, BLK), jnp.float32),
            pltpu.VMEM((4, 8, 1, BLK), jnp.float32),
            pltpu.VMEM((8, 2 * BLK, BLK), jnp.float32),
            pltpu.SemaphoreType.DMA((2,)),
            pltpu.SemaphoreType.DMA,
            pltpu.SemaphoreType.DMA((6,)),
            pltpu.SemaphoreType.DMA((COPIES,)),
            pltpu.SemaphoreType.DMA((4, 4, 2)),
        ],
        compiler_params=pltpu.CompilerParams(
            collective_id=number, has_side_effects=True, vmem_limit_bytes=48 * 1024 * 1024
        ),
        cost_estimate=pl.CostEstimate(
            flops=2 * cap * 1024 * 1024, bytes_accessed=3 << 20, transcendentals=0
        ),
        name=f"wgrad{number}",
    )


def shards(attn_out, out_grad, valid_counts):
    hbm = pl.BlockSpec(memory_space=pltpu.HBM)
    vmem = pl.BlockSpec(memory_space=pltpu.VMEM)
    grains = [value.reshape(TOK // GRAIN, GRAIN, BLK) for value in (attn_out, out_grad)]
    turned, packed, which = pl.pallas_call(
        compact,
        out_shape=(
            jax.ShapeDtypeStruct((BLK, TOK), attn_out.dtype),
            jax.ShapeDtypeStruct((TOK, BLK), out_grad.dtype),
            jax.ShapeDtypeStruct((1,), jnp.int32),
        ),
        in_specs=[hbm, hbm, hbm],
        out_specs=(vmem, vmem, pl.BlockSpec(memory_space=pltpu.SMEM)),
        scratch_shapes=[
            pltpu.SMEM((TOK // SEQ,), jnp.int32),
            pltpu.VMEM((TOK // GRAIN, GRAIN, BLK), jnp.bfloat16),
            pltpu.VMEM((TOK // GRAIN, GRAIN, BLK), jnp.bfloat16),
            pltpu.VMEM((8, BLK), jnp.int32),
            pltpu.VMEM((3, 8, BLK), jnp.int32),
            pltpu.SemaphoreType.DMA,
            pltpu.SemaphoreType.DMA((2, TOK // SEQ)),
            pltpu.SemaphoreType.DMA((3,)),
            pltpu.SemaphoreType.DMA((3,)),
        ],
        compiler_params=pltpu.CompilerParams(
            collective_id=0, has_side_effects=True, vmem_limit_bytes=16 * 1024 * 1024
        ),
        name="compact",
    )(*(pltpu.with_memory_space_constraint(value, pltpu.HBM) for value in (valid_counts, *grains)))
    branches = [main(plan, 1 + i) for i, plan in enumerate(PLANS)]
    return lax.switch(which[0], branches, turned, packed)


def solution(mesh):
    return jax.shard_map(
        shards,
        mesh=mesh,
        in_specs=(P("gx", ("gy", "gz")), P("gx", ("gz", "gy")), P("gx")),
        out_specs=P(("gy", "gx"), "gz"),
        check_vma=False,
    )
```

```python
import functools

import jax
import jax.numpy as jnp
from jax import lax
from jax.experimental import pallas as pl
from jax.experimental.pallas import tpu as pltpu
from jax.sharding import PartitionSpec as P

MESH = pl.DeviceIdType.MESH
TOK = 4096
SEQ = 1024
BLK = 128
GRAIN = 16
PLANS = (
    (2432, 2304, 2304, 2432), (2176, 2688, 2688, 2176), (2688, 2688, 1920, 2688), (2560, 2432, 2560, 2560),
    (2432, 2432, 2816, 2816), (2816, 2816, 2432, 2432), (2304, 2944, 2944, 2944), (2944, 2944, 2944, 2304),
    (2944, 2688, 2688, 2944), (3072, 3072, 3072, 2688), (2688, 3072, 3072, 3072), (3200, 3200, 3200, 3200),
    (3328, 3328, 3328, 3328), (3456, 3456, 3456, 3456), (3712, 3712, 3712, 3712), (4096, 4096, 4096, 4096),
)
UNROLL = 4
COPIES = 37


def compact(vc_hbm, a_hbm, b_hbm, at_out, b_out, which, vc, raw_a, raw_b, mine, theirs, csem, lsem, ss, rs):
    zl = lax.axis_index("gx")
    gy = lax.axis_index("gy")
    gz = lax.axis_index("gz")
    rows_here = TOK // SEQ
    barrier = pltpu.get_barrier_semaphore()
    peers = [((zl + d) % 4, gy, gz) for d in range(1, 4)]
    for dev in peers:
        pl.semaphore_signal(barrier, inc=1, device_id=dev, device_id_type=MESH)
    counts = pltpu.make_async_copy(vc_hbm, vc, csem)
    counts.start()
    loads = []
    for r in range(rows_here):
        part = pl.ds(r * (SEQ // GRAIN), SEQ // GRAIN)
        loads.append(pltpu.make_async_copy(a_hbm.at[part], raw_a.at[part], lsem.at[0, r]))
        loads.append(pltpu.make_async_copy(b_hbm.at[part], raw_b.at[part], lsem.at[1, r]))
    for load in loads:
        load.start()
    counts.wait()
    valid = [vc[r] for r in range(rows_here)]
    first = [0]
    for r in range(rows_here):
        first.append(first[-1] + (valid[r] + GRAIN - 1) // GRAIN)
    mine[...] = jnp.full(mine.shape, first[-1] * GRAIN, jnp.int32)
    pl.semaphore_wait(barrier, len(peers))
    copies = [
        pltpu.make_async_remote_copy(
            src_ref=mine, dst_ref=theirs.at[d], send_sem=ss.at[d], recv_sem=rs.at[d],
            device_id=peers[d], device_id_type=MESH,
        )
        for d in range(3)
    ]
    for copy in copies:
        copy.start()
    for load in loads:
        load.wait()

    shift = [r * (SEQ // GRAIN) - first[r] for r in range(rows_here)]
    limit = [valid[r] + first[r] * GRAIN for r in range(rows_here)]
    token = lax.broadcasted_iota(jnp.int32, (GRAIN, BLK), 0)

    def tile(k):
        pieces = []
        for i in range(BLK // GRAIN):
            n = k * (BLK // GRAIN) + i
            move, end = shift[0], limit[0]
            for r in range(1, rows_here):
                past = n >= first[r]
                move = jnp.where(past, shift[r], move)
                end = jnp.where(past, limit[r], end)
            source = jnp.minimum(n + move, TOK // GRAIN - 1)
            piece = raw_a[source]
            pieces.append(jnp.where(token < end - n * GRAIN, piece, jnp.zeros((), piece.dtype)))
            b_out[pl.ds(pl.multiple_of(n * GRAIN, GRAIN), GRAIN), :] = raw_b[source]
        span = pl.ds(pl.multiple_of(k * BLK, BLK), BLK)
        at_out[:, span] = jnp.concatenate(pieces, axis=0).T

    def tiles(k, carry):
        for i in range(UNROLL):
            tile(k * UNROLL + i)
        return carry

    lax.fori_loop(0, TOK // BLK // UNROLL, tiles, 0)
    for copy in copies:
        copy.wait_recv()
    totals = [first[-1] * GRAIN] + [theirs[d, 0, 0] for d in range(3)]
    group = []
    for g in range(4):
        back, value = (zl + 4 - g) % 4, totals[3]
        for d in range(3):
            value = jnp.where(back == d, totals[d], value)
        group.append(value)
    index = len(PLANS) - 1
    for n in reversed(range(len(PLANS) - 1)):
        short = sum(jnp.where(group[g] > PLANS[n][g], 1, 0) for g in range(4))
        index = jnp.where(short == 0, n, index)
    which[0] = index
    for copy in copies:
        copy.wait_send()


def kernel(plan, a_hbm, b_hbm, result, out, at, bb, sbuf, rbuf, ssc, rsc, acc, lsem, osem, sent, rs, prs):
    cap, low = max(plan), min(plan)
    CHK, HALF = low // 4, cap // 2
    zl = lax.axis_index("gx")
    gy = lax.axis_index("gy")
    gz = lax.axis_index("gz")
    x, zh = gy // 2, gy % 2
    y, c = gz // 2, gz % 2
    xr, xl, xo = (x + 1) % 4, (x + 3) % 4, (x + 2) % 4
    yr, yl, yo = (y + 1) % 4, (y + 3) % 4, (y + 2) % 4

    right, left = (zl, xr * 2 + zh, gz), (zl, xl * 2 + zh, gz)
    far = (zl, x * 2 + (1 - zh), gz)
    up, down = (zl, gy, yr * 2 + c), (zl, gy, yl * 2 + c)
    sibling = (zl, gy, y * 2 + (1 - c))
    owners = [((zl + d) % 4, gy, gz) for d in range(1, 4)]

    barrier = pltpu.get_barrier_semaphore()
    partners = [far, right, left, up, down, sibling] + owners
    for dev in partners:
        pl.semaphore_signal(barrier, inc=1, device_id=dev, device_id_type=MESH)

    def rows(block, h=None):
        if h is None:
            return pl.ds(pl.multiple_of(block * BLK, BLK), BLK)
        return pl.ds(pl.multiple_of(block * BLK + h * (BLK // 2), BLK // 2), BLK // 2)

    load_a = pltpu.make_async_copy(a_hbm.at[:, pl.ds(0, cap)], at.at[rows(gz)], lsem.at[0])
    load_b = pltpu.make_async_copy(b_hbm.at[pl.ds(0, cap)], bb.at[gy], lsem.at[1])
    load_a.start()
    load_b.start()
    pl.semaphore_wait(barrier, len(partners))

    made = []

    def remote(src, dst, dev, kind=4):
        k = len(made)
        copy = pltpu.make_async_remote_copy(
            src_ref=src,
            dst_ref=dst,
            send_sem=sent.at[kind],
            recv_sem=rs.at[k],
            device_id=dev,
            device_id_type=MESH,
        )
        made.append(copy)
        return copy

    def tokens(q, size):
        return pl.ds(q * size, size)

    far_q = {q: remote(b_hbm.at[tokens(q, CHK)], bb.at[gy, tokens(q, CHK)], far) for q in range(4)}
    own_r = {h: remote(b_hbm.at[tokens(h, HALF)], bb.at[gy, tokens(h, HALF)], right, 0) for h in range(2)}
    own_l = {h: remote(b_hbm.at[tokens(h, HALF)], bb.at[gy, tokens(h, HALF)], left, 0) for h in range(2)}

    def relay(slot, q, size, dev, kind=4):
        return remote(bb.at[slot, tokens(q, size)], bb.at[slot, tokens(q, size)], dev, kind)

    hop_r = relay(xl * 2 + zh, 0, HALF, right, 0)
    hop_l = relay(xr * 2 + zh, 1, HALF, left, 0)
    oz = 1 - zh
    far_r = {q: relay(x * 2 + oz, q, CHK, right) for q in range(4)}
    far_l = {q: relay(x * 2 + oz, q, CHK, left) for q in range(4)}
    fhop_r = {q: relay(xl * 2 + oz, q, CHK, right) for q in (0, 1)}
    fhop_l = {q: relay(xr * 2 + oz, q, CHK, left) for q in (2, 3)}

    tail = pl.ds(low, cap - low)
    large = functools.reduce(jnp.logical_or, [zl == g for g in range(4) if plan[g] == cap])

    def larger(do):
        if low < cap:
            pl.when(large)(do)

    def more(slot, begin, size, dev):
        part = pl.ds(begin, size)
        return remote(bb.at[slot, part], bb.at[slot, part], dev, 5)

    if low < cap:
        rest = (cap - low) // 2
        tail_far = remote(b_hbm.at[tail], bb.at[gy, tail], far, 5)
        tail_r = more(x * 2 + oz, low, cap - low, right)
        tail_l = more(x * 2 + oz, low, cap - low, left)
        tail_hop_r = more(xl * 2 + oz, low, rest, right)
        tail_hop_l = more(xr * 2 + oz, low + rest, rest, left)

    def pass_on(block, h, dev):
        return remote(at.at[rows(block, h)], at.at[rows(block, h)], dev, 1)

    def own(h, dev):
        part = pl.ds(h * (BLK // 2), BLK // 2)
        return remote(a_hbm.at[part, pl.ds(0, cap)], at.at[rows(gz, h)], dev, 1)

    a_up = {h: own(h, up) for h in range(2)}
    a_down = {h: own(h, down) for h in range(2)}
    ahop_up = pass_on(yl * 2 + c, 0, up)
    ahop_down = pass_on(yr * 2 + c, 1, down)
    sib = {d: pass_on(((y + d) % 4) * 2 + c, None, sibling) for d in range(1, 4)}
    sib[0] = remote(a_hbm.at[:, pl.ds(0, cap)], at.at[rows(gz)], sibling, 1)

    for q in (0, 2, 1, 3):
        far_q[q].start()

    @larger
    def _():
        tail_far.start()

    own_r[0].start()
    own_l[1].start()
    own_r[1].start()
    own_l[0].start()

    a_up[0].start()
    a_down[1].start()
    a_up[1].start()
    a_down[0].start()
    sib[0].start()

    if low < cap:

        @pl.when(jnp.logical_not(large))
        def _():
            def blank(n, carry):
                part = pl.ds(pl.multiple_of(low + n * BLK, BLK), BLK)
                for v in range(4):
                    bb[v * 2 + oz, part, :] = jnp.zeros((BLK, BLK), bb.dtype)
                return carry

            lax.fori_loop(0, (cap - low) // BLK, blank, 0)

    own_r[0].wait_recv()
    hop_r.start()
    own_l[1].wait_recv()
    hop_l.start()
    a_up[0].wait_recv()
    ahop_up.start()
    a_down[1].wait_recv()
    ahop_down.start()
    far_q[0].wait_recv()
    far_r[0].start()
    far_l[0].start()
    a_up[1].wait_recv()
    sib[3].start()
    a_down[0].wait_recv()
    sib[1].start()
    far_q[2].wait_recv()
    far_r[2].start()
    far_l[2].start()
    ahop_up.wait_recv()
    ahop_down.wait_recv()
    sib[2].start()
    far_q[1].wait_recv()
    far_r[1].start()
    far_l[1].start()
    for d in range(4):
        sib[d].wait_recv()

    side = zl // 2
    mid = (zl + side) % 2
    end_at, mid_at, far_mid, far_end = 3 * side, 1 + side, 2 - side, 3 - 3 * side
    goal = [
        mid * far_mid + (1 - mid) * far_end,
        mid * end_at + (1 - mid) * far_mid,
        mid * far_end + (1 - mid) * mid_at,
    ]
    goes_to = [
        mid * far_mid + (1 - mid) * mid_at,
        mid * end_at + (1 - mid) * far_mid,
        mid * far_end + (1 - mid) * mid_at,
    ]
    lands = [3 * (1 - mid), 1 - mid, 2 - mid]

    blocks = [gy, xr * 2 + zh, xl * 2 + zh, xo * 2 + zh, x * 2 + oz, xr * 2 + oz, xl * 2 + oz, xo * 2 + oz]

    def pick(choices, k):
        if isinstance(k, int):
            return choices[k]
        value = choices[-1]
        for i in range(len(choices) - 1):
            value = jnp.where(k == i, choices[i], value)
        return value

    def part_copies(k, u, slot):
        span = pl.ds(2 * u, 2)
        dev = (pick(goes_to, k), gy, gz)
        return [
            pltpu.make_async_remote_copy(
                src_ref=src.at[k, span],
                dst_ref=dst.at[slot, span],
                send_sem=sent.at[2 + w],
                recv_sem=prs.at[slot, u, w],
                device_id=dev,
                device_id_type=MESH,
            )
            for w, (src, dst) in enumerate(((sbuf, rbuf), (ssc, rsc)))
        ]

    def columns(u, i):
        return pl.ds(pl.multiple_of(pick(blocks[i::2], u) * BLK, BLK), BLK)

    def product(chunk, u):
        lhs = at[pl.ds(pl.multiple_of(chunk * 2 * BLK, 2 * BLK), 2 * BLK), :]
        rhs = jnp.concatenate([bb[pick(blocks[i::2], u)] for i in range(2)], axis=1)
        part = jnp.dot(lhs, rhs, preferred_element_type=jnp.float32)
        return [part[:, :BLK], part[:, BLK:]]

    def send(k, u, parts):
        for i in range(2):
            top = jnp.maximum(jnp.max(jnp.abs(parts[i]), axis=0, keepdims=True), 2e-34)
            sbuf[k, 2 * u + i] = jnp.round(parts[i] * (32767.0 / top)).astype(jnp.int32).astype(jnp.int16)
            ssc[k, 2 * u + i] = top * (1.0 / 32767.0)
        for copy in part_copies(k, u, pick(lands, k)):
            copy.start()

    def arrived(slot, u):
        for copy in part_copies(0, u, slot):
            copy.wait_recv()
        return [
            rbuf[slot, 2 * u + i].astype(jnp.int32).astype(jnp.float32) * rsc[slot, 2 * u + i]
            for i in range(2)
        ]

    def unit(u):
        def step(k, carry):
            parts = product(pick(goal + [zl], k), u)
            held = jnp.logical_and(k == 2, mid == 1)

            @pl.when(jnp.logical_and(k < 3, jnp.logical_not(held)))
            def _():
                send(k, u, parts)

            @pl.when(held)
            def _():
                for i in range(2):
                    acc[2 * u + i] = parts[i]

            @pl.when(k == 3)
            def _():
                for i in range(2):
                    out[:, columns(u, i)] = parts[i]

            return carry

        lax.fori_loop(0, 4, step, 0)

    def finish(u):
        parts = arrived(3, u)
        send(2, u, [acc[2 * u + i] + parts[i] for i in range(2)])

    def stores(u):
        return [
            pltpu.make_async_copy(out.at[:, columns(u, i)], result.at[:, columns(u, i)], osem)
            for i in range(2)
        ]

    def gather(u, carry):
        def add(slot):
            parts = arrived(slot, u)
            for i in range(2):
                out[:, columns(u, i)] += parts[i]

        add(0)

        @pl.when(mid == 1)
        def _():
            add(2)

        add(1)
        for copy in stores(u):
            copy.start()
        return carry

    def stage(u, carry):
        @pl.when(u == 0)
        def _():
            load_a.wait()
            load_b.wait()
            own_l[0].wait_recv()

        @pl.when(u == 1)
        def _():
            far_q[3].wait_recv()
            far_r[3].start()
            far_l[3].start()

            @larger
            def _():
                tail_far.wait_recv()
                tail_r.start()
                tail_l.start()

            far_r[0].wait_recv()
            fhop_r[0].start()
            far_l[2].wait_recv()
            fhop_l[2].start()
            own_r[1].wait_recv()
            hop_r.wait_recv()
            hop_l.wait_recv()

        @pl.when(u == 2)
        def _():
            far_r[1].wait_recv()
            fhop_r[1].start()
            far_l[3].wait_recv()
            fhop_l[3].start()
            far_l[0].wait_recv()
            far_l[1].wait_recv()

            @larger
            def _():
                tail_r.wait_recv()
                tail_hop_r.start()
                tail_l.wait_recv()
                tail_hop_l.start()


        @pl.when(u == 3)
        def _():
            far_r[2].wait_recv()
            far_r[3].wait_recv()
            fhop_r[0].wait_recv()
            fhop_r[1].wait_recv()
            fhop_l[2].wait_recv()
            fhop_l[3].wait_recv()

            @larger
            def _():
                tail_hop_r.wait_recv()
                tail_hop_l.wait_recv()

        unit(u)

        @pl.when(jnp.logical_and(u > 0, mid == 1))
        def _():
            finish(u - 1)

        return carry

    lax.fori_loop(0, 4, stage, 0)

    @pl.when(mid == 1)
    def _():
        finish(3)

    lax.fori_loop(0, 4, gather, 0)
    pltpu.make_async_copy(out, result, osem).wait()
    exchanged = bb.at[pl.ds(0, 4), pl.ds(0, low)]
    pltpu.make_async_copy(bb.at[pl.ds(0, 3)], bb.at[pl.ds(0, 3)], sent.at[0]).wait()
    pltpu.make_async_copy(exchanged, exchanged, sent.at[4]).wait()

    @larger
    def _():
        beyond = bb.at[pl.ds(0, 4), tail]
        pltpu.make_async_copy(beyond, beyond, sent.at[5]).wait()

    pltpu.make_async_copy(at.at[pl.ds(0, 7 * BLK)], at.at[pl.ds(0, 7 * BLK)], sent.at[1]).wait()
    pltpu.make_async_copy(sbuf, sbuf, sent.at[2]).wait()
    pltpu.make_async_copy(ssc, ssc, sent.at[3]).wait()


def main(plan, number):
    cap = max(plan)
    any_space = pl.BlockSpec(memory_space=pl.ANY)
    return pl.pallas_call(
        functools.partial(kernel, plan),
        out_shape=jax.ShapeDtypeStruct((2 * BLK, 8 * BLK), jnp.float32),
        in_specs=[any_space] * 2,
        out_specs=any_space,
        scratch_shapes=[
            pltpu.VMEM((2 * BLK, 8 * BLK), jnp.float32),
            pltpu.VMEM((8 * BLK, cap), jnp.bfloat16),
            pltpu.VMEM((8, cap, BLK), jnp.bfloat16),
            pltpu.VMEM((3, 8, 2 * BLK, BLK), jnp.int16),
            pltpu.VMEM((4, 8, 2 * BLK, BLK), jnp.int16),
            pltpu.VMEM((3, 8, 1, BLK), jnp.float32),
            pltpu.VMEM((4, 8, 1, BLK), jnp.float32),
            pltpu.VMEM((8, 2 * BLK, BLK), jnp.float32),
            pltpu.SemaphoreType.DMA((2,)),
            pltpu.SemaphoreType.DMA,
            pltpu.SemaphoreType.DMA((6,)),
            pltpu.SemaphoreType.DMA((COPIES,)),
            pltpu.SemaphoreType.DMA((4, 4, 2)),
        ],
        compiler_params=pltpu.CompilerParams(
            collective_id=number, has_side_effects=True, vmem_limit_bytes=48 * 1024 * 1024
        ),
        cost_estimate=pl.CostEstimate(
            flops=2 * cap * 1024 * 1024, bytes_accessed=3 << 20, transcendentals=0
        ),
        name=f"wgrad{number}",
    )


def shards(attn_out, out_grad, valid_counts):
    hbm = pl.BlockSpec(memory_space=pltpu.HBM)
    vmem = pl.BlockSpec(memory_space=pltpu.VMEM)
    grains = [value.reshape(TOK // GRAIN, GRAIN, BLK) for value in (attn_out, out_grad)]
    turned, packed, which = pl.pallas_call(
        compact,
        out_shape=(
            jax.ShapeDtypeStruct((BLK, TOK), attn_out.dtype),
            jax.ShapeDtypeStruct((TOK, BLK), out_grad.dtype),
            jax.ShapeDtypeStruct((1,), jnp.int32),
        ),
        in_specs=[hbm, hbm, hbm],
        out_specs=(vmem, vmem, pl.BlockSpec(memory_space=pltpu.SMEM)),
        scratch_shapes=[
            pltpu.SMEM((TOK // SEQ,), jnp.int32),
            pltpu.VMEM((TOK // GRAIN, GRAIN, BLK), jnp.bfloat16),
            pltpu.VMEM((TOK // GRAIN, GRAIN, BLK), jnp.bfloat16),
            pltpu.VMEM((8, BLK), jnp.int32),
            pltpu.VMEM((3, 8, BLK), jnp.int32),
            pltpu.SemaphoreType.DMA,
            pltpu.SemaphoreType.DMA((2, TOK // SEQ)),
            pltpu.SemaphoreType.DMA((3,)),
            pltpu.SemaphoreType.DMA((3,)),
        ],
        compiler_params=pltpu.CompilerParams(
            collective_id=0, has_side_effects=True, vmem_limit_bytes=16 * 1024 * 1024
        ),
        name="compact",
    )(*(pltpu.with_memory_space_constraint(value, pltpu.HBM) for value in (valid_counts, *grains)))
    branches = [main(plan, 1 + i) for i, plan in enumerate(PLANS)]
    return lax.switch(which[0], branches, turned, packed)


def solution(mesh):
    return jax.shard_map(
        shards,
        mesh=mesh,
        in_specs=(P("gx", ("gy", "gz")), P("gx", ("gz", "gy")), P("gx")),
        out_specs=P(("gy", "gx"), "gz"),
        check_vma=False,
    )
```
